256 devices in a mesh: phi: 32 (over z, x_hi, core), eta: 8 (over y, x_lo).
Axes of the slice: x: 4 (x_hi: 2, x_lo: 2; x = x_hi * 2 + x_lo), y: 4, z: 8, core: 2. Of those that a mesh axis runs over, the one named last changes fastest.
Arguments:
- features: bfloat16 [32, 512, 1024], P(None, 'phi', 'eta'), may hold values from -6 to 6
- cotangent: bfloat16 [32, 512, 1024], P(None, 'phi', 'eta'), may hold values from -6 to 6
- kernel_a: bfloat16 [27, 32, 32], replicated, may hold values from -0.21875 to 0.21875
- kernel_b: bfloat16 [27, 64, 32], replicated, may hold values from -0.21875 to 0.21875
- mixing: bfloat16 [32, 64], replicated, may hold values from -0.75 to 0.75
Outputs:
- output: bfloat16 [32, 512, 1024], P(None, 'phi', 'eta')
- grad_input: bfloat16 [32, 512, 1024], P(None, 'phi', 'eta')
- grad_kernel_a: float32 [27, 32, 32], replicated
- grad_kernel_b: float32 [27, 64, 32], replicated
- grad_mixing: float32 [32, 64], replicated
The draws below stay inside these ranges and needn't reach their ends.
All inputs are finite; a program needn't handle non-finite values.
Results may differ from the reference program's by a relative error of at most 0.012.
Values may be sent and summed in bfloat16 or wider, within the bound.
A program may use at most 128 MiB of HBM per device.

```python
import jax
import jax.numpy as jnp
from jax import lax

C1 = 32
C2 = 64
LAYERS = 32
PHI = 512
ETA = 32


def block_levels(stream_key, dims, cuts, smallest, top_value):
    def one(position, shards_of):
        steps = jax.random.uniform(jax.random.fold_in(jax.random.fold_in(stream_key, 6), position), (shards_of,), jnp.float32, smallest / len(cuts), top_value / len(cuts))
        return jnp.repeat(jnp.exp(steps), dims[position] // shards_of).reshape((-1,) + (1,) * (len(dims) - position - 1))

    factor_of = one(*cuts[0])
    for cut in cuts[1:]:
        factor_of = factor_of * one(*cut)
    return factor_of


def noise(stream_key, shape, scale, bound, split=(), dtype=jnp.bfloat16):
    result = scale * jax.random.normal(stream_key, shape, jnp.float32)
    if split:
        result = result * block_levels(stream_key, shape, split, -0.22, 0.18)
    return jnp.clip(result, -bound, bound).astype(dtype)


def setup_inputs(seed: int = 0) -> dict:
    arg_keys = jax.random.split(jax.random.key(seed), 6)
    features = noise(arg_keys[0], (C1, PHI, ETA * LAYERS), 1.0, 6.0, ((1, 32), (2, 8)))
    cotangent = noise(arg_keys[1], (C1, PHI, ETA * LAYERS), 1.0, 6.0, ((1, 32), (2, 8)))
    kernel_a = noise(arg_keys[2], (27, C1, C1), (27 * C1) ** -0.5, 0.21875)
    kernel_b = noise(arg_keys[3], (27, C2, C1), (27 * C1) ** -0.5, 0.21875)
    mixing = noise(arg_keys[4], (C1, C2), C2 ** -0.5, 0.75)
    return {"features": features, "cotangent": cotangent, "kernel_a": kernel_a, "kernel_b": kernel_b, "mixing": mixing}


def wrap_pad(values):
    looped = jnp.concatenate([values[:, -1:], values, values[:, :1]], axis=1)
    return jnp.pad(looped, ((0, 0), (0, 0), (1, 1), (1, 1)))

def shifted(padded, offset, extent):
    step_phi = offset // 9
    step_eta = offset // 3 % 3
    step_layer = offset % 3
    window = padded[:, step_phi:step_phi + extent[0], step_eta:step_eta + extent[1], step_layer:step_layer + extent[2]]
    return window.reshape(padded.shape[0], -1)

def convolve(padded, weight):
    extent = (padded.shape[1] - 2, padded.shape[2] - 2, padded.shape[3] - 2)
    summed = jnp.zeros((weight.shape[1], extent[0] * extent[1] * extent[2]), jnp.float32)
    for offset in range(27):
        summed = summed + jnp.dot(weight[offset], shifted(padded, offset, extent), preferred_element_type=jnp.float32)
    return summed.reshape((weight.shape[1],) + extent)

def kernel_grad(padded, upstream):
    extent = upstream.shape[1:]
    flat_up = upstream.reshape(upstream.shape[0], -1)
    kernel_terms = [lax.dot_general(flat_up, shifted(padded, offset, extent), (((1,), (1,)), ((), ())), preferred_element_type=jnp.float32) for offset in range(27)]
    return jnp.stack(kernel_terms)

def flipped(weight):
    return jnp.transpose(weight[::-1], (0, 2, 1))

def block_view(fine_grid):
    chans, rows_phi, rows_eta, layer_count = fine_grid.shape
    return fine_grid.astype(jnp.float32).reshape(chans, rows_phi // 2, 2, rows_eta // 2, 2, layer_count)

def widened(coarse):
    return jnp.repeat(jnp.repeat(coarse, 2, axis=1), 2, axis=2)

def silu_slope(linear):
    logistic = jax.nn.sigmoid(linear)
    return logistic * (1.0 + linear * (1.0 - logistic))

def mix_channels(mixing, gated):
    flat_gated = gated.reshape(gated.shape[0], -1)
    mixed = jnp.dot(mixing, flat_gated, preferred_element_type=jnp.float32)
    return mixed.reshape((mixing.shape[0],) + gated.shape[1:])

def unfold(field):
    return field.reshape(field.shape[0], field.shape[1], -1, LAYERS)

def refold(field):
    return field.reshape(field.shape[0], field.shape[1], -1)

def reference(features, cotangent, kernel_a, kernel_b, mixing):
    features = unfold(features)
    cotangent = unfold(cotangent)
    fine_pad = wrap_pad(features)
    linear_a = convolve(fine_pad, kernel_a)
    hidden = jax.nn.silu(linear_a).astype(jnp.bfloat16)
    coarse = block_view(hidden).mean(axis=(2, 4)).astype(jnp.bfloat16)
    coarse_pad = wrap_pad(coarse)
    linear_b = convolve(coarse_pad, kernel_b)
    gated = jax.nn.silu(linear_b).astype(jnp.bfloat16)
    projected = mix_channels(mixing, gated).astype(jnp.bfloat16)
    output = (hidden.astype(jnp.float32) + widened(projected.astype(jnp.float32))).astype(jnp.bfloat16)
    folded = block_view(cotangent).sum(axis=(2, 4)).astype(jnp.bfloat16)
    flat_folded = folded.reshape(folded.shape[0], -1)
    mix_sum = lax.dot_general(flat_folded, gated.reshape(gated.shape[0], -1), (((1,), (1,)), ((), ())), preferred_element_type=jnp.float32)
    grad_gated = lax.dot_general(mixing, flat_folded, (((0,), (0,)), ((), ())), preferred_element_type=jnp.float32).reshape(linear_b.shape)
    grad_linear_b = (grad_gated * silu_slope(linear_b)).astype(jnp.bfloat16)
    kernel_b_sum = kernel_grad(coarse_pad, grad_linear_b)
    grad_coarse = convolve(wrap_pad(grad_linear_b), flipped(kernel_b)).astype(jnp.bfloat16)
    grad_hidden = cotangent.astype(jnp.float32) + 0.25 * widened(grad_coarse.astype(jnp.float32))
    grad_linear_a = (grad_hidden * silu_slope(linear_a)).astype(jnp.bfloat16)
    kernel_a_sum = kernel_grad(fine_pad, grad_linear_a)
    grad_input = convolve(wrap_pad(grad_linear_a), flipped(kernel_a)).astype(jnp.bfloat16)
    factor = 1.0 / jnp.sqrt(jnp.float32(features.shape[1] * features.shape[2] * features.shape[3]))
    return (refold(output), refold(grad_input), kernel_a_sum * factor, kernel_b_sum * factor, mix_sum * factor)
```

```python
import functools
import math

import jax
import jax.numpy as jnp
from jax import lax
from jax.experimental import pallas as pl
from jax.experimental.pallas import tpu as pltpu
from jax.sharding import PartitionSpec as P

BF = jnp.bfloat16
F32 = jnp.float32
MESH = pl.DeviceIdType.MESH
DIRS = ((0, 1), (0, -1), (1, 0), (1, 1), (1, -1), (-1, 0), (-1, 1), (-1, -1))
A_TILES = 14
B_TILES = 28


def lane_of(shape):
    return lax.broadcasted_iota(jnp.int32, shape, len(shape) - 1)


def roll(x, shift):
    shift %= 128
    return x if shift == 0 else pltpu.roll(x, shift, x.ndim - 1)


def dot(a, b):
    return jnp.dot(a, b, preferred_element_type=F32)


def dot_nt(a, b):
    return lax.dot_general(a, b, (((1,), (1,)), ((), ())), preferred_element_type=F32)


def zero(x):
    return jnp.zeros((), x.dtype)


def side_by_side(rows):
    return jnp.concatenate(rows, axis=1)


def by_quarter(v0, v1, v2, v3):
    lane = lane_of(v0.shape)
    return jnp.where(
        lane < 64, jnp.where(lane < 32, v0, v1), jnp.where(lane < 96, v2, v3)
    )


def pack_column(x, size, start):
    return by_quarter(
        *[roll(x[size * g : size * (g + 1)], 32 * g - start) for g in range(4)]
    )


def unpack_column(packed, want):
    return [roll(packed, want - 32 * g) for g in range(4)]


def pack_pair(x, y):
    return jnp.where(lane_of(x.shape) < 64, roll(x, -32), roll(y, 32))


def widen_columns(x):
    lane = lane_of(x.shape)
    return jnp.where(lane < 32, roll(x, -32), jnp.where(lane < 96, x, roll(x, 32)))


def pool_columns(x):
    lane = lane_of(x.shape)
    both = x + jnp.where(lane < 64, roll(x, 32), roll(x, -32))
    return jnp.where((lane >= 32) & (lane < 96), both, zero(x))


def layer_shifts(x):
    layer = lane_of(x.shape) % 32
    return [
        jnp.where(layer < 31, roll(x, -1), zero(x)),
        x,
        jnp.where(layer > 0, roll(x, 1), zero(x)),
    ]


def conv_rows(src, count, weight, outs, sink):
    layer = lane_of((outs, 128)) % 32
    flat = 3 * src.shape[1]
    for r in range(0, count, 2):
        pair = [src[r + i : r + i + 3].reshape(flat, 128) for i in range(2)]
        z = dot(weight, side_by_side(pair))
        for i in range(2):
            zi = z[:, 128 * i : 128 * (i + 1)]
            low = jnp.where(layer > 0, roll(zi[:outs], 1), 0.0)
            high = jnp.where(layer < 31, roll(zi[2 * outs :], -1), 0.0)
            sink[r + i] = zi[outs : 2 * outs] + low + high


def sigmoid(v):
    return 1.0 / (1.0 + jnp.exp(-v))


def kernel(n_phi, n_eta, scale, *refs):
    (f_ref, ct_ref, ka_ref, kb_ref, mix_ref, out_ref, gi_ref, gka_ref, gkb_ref, gm_ref) = refs[:10]
    (
        x_s, colx_s, rcx, rrx,
        fold_s, colf_s, rcf, rrf,
        colc_s, rowc_s, rcc, rrc,
        g_s, colg_s, rcg, rrg,
        sfa, scb, sgb, sga, lin_a_s, lin_b_s, gc_s, gi_s,
        pa, ra1, xa2, ra2, xa3, resa,
        pb, rb1, xb2, rb2, xb3, resb,
        h_send, h_recv, a_send, a_recv, b_send, b_recv,
    ) = refs[10:]
    p = lax.axis_index("phi")
    e = lax.axis_index("eta")
    g1, g2 = 2 * n_eta, n_phi // 2
    hi_bit = lax.rem(p // 2, 2)
    me1 = hi_bit * n_eta + e
    me2 = (p // 4) * 2 + lax.rem(p, 2)

    def halo_device(d):
        return (lax.rem(p + d[0] + n_phi, n_phi), lax.rem(e + d[1] + n_eta, n_eta))

    def plane_device(i):
        q = lax.rem(me1 + i, g1)
        return ((p // 4) * 4 + (q // n_eta) * 2 + lax.rem(p, 2), lax.rem(q, n_eta))

    def line_device(i):
        r = lax.rem(me2 + i, g2)
        return ((r // 2) * 4 + hi_bit * 2 + lax.rem(r, 2), e)

    barrier = pltpu.get_barrier_semaphore()
    targets = [halo_device(d) for d in DIRS]
    targets += [plane_device(i) for i in range(1, g1)]
    targets += [line_device(i) for i in range(1, g2)]
    for target in targets:
        pl.semaphore_signal(barrier, inc=1, device_id=target, device_id_type=MESH)

    pending = []

    def send(src, dst, ssem, rsem, target):
        copy = pltpu.make_async_remote_copy(
            src_ref=src, dst_ref=dst, send_sem=ssem, recv_sem=rsem,
            device_id=target, device_id_type=MESH,
        )
        copy.start()
        pending.append(copy)
        return copy

    def halo_start(which, cols, rows, rc, rr):
        copies = []
        for k, d in enumerate(DIRS):
            if k < 2:
                src, dst = cols[k], rc.at[k]
            else:
                src, dst = rows[0 if d[0] > 0 else 1], rr.at[k - 2]
            copies.append(send(src, dst, h_send.at[which, k], h_recv.at[which, k], halo_device(d)))
        return copies

    def halo_wait(copies):
        for copy in copies:
            copy.wait_recv()

    has_left = e > 0
    has_right = e < n_eta - 1
    lo32 = jnp.where(has_left, 32, 0)
    lo64 = jnp.where(has_left, 64, 0)
    hi96 = jnp.where(has_right, 96, 128)
    hi64 = jnp.where(has_right, 64, 128)

    x = jnp.transpose(f_ref[...], (1, 0, 2))
    x_s[...] = x
    colx_s[0] = pack_column(x, 4, 96)
    colx_s[1] = pack_column(x, 4, 0)
    pl.semaphore_wait(barrier, len(targets))
    halo_x = halo_start(
        0, (colx_s.at[0], colx_s.at[1]), (x_s.at[15], x_s.at[0]), rcx, rrx
    )

    ct = jnp.transpose(ct_ref[...], (1, 0, 2)).astype(F32).reshape(8, 2, 32, 128)
    fold = pool_columns(ct[:, 0] + ct[:, 1]).astype(BF)
    fold_s[...] = fold
    colf_s[0] = pack_column(fold, 2, 64)
    colf_s[1] = pack_column(fold, 2, 32)
    halo_f = halo_start(
        1, (colf_s.at[0], colf_s.at[1]), (fold_s.at[7], fold_s.at[0]), rcf, rrf
    )

    def forward_weight(ref):
        return jnp.concatenate(
            [side_by_side([ref[3 * ab + c] for ab in range(9)]) for c in range(3)], axis=0
        )

    def backward_weight(ref):
        return jnp.concatenate(
            [side_by_side([ref[26 - 3 * ab - c] for c in range(3)]) for ab in range(9)], axis=0
        ).T

    wa_f, wb_f = forward_weight(ka_ref), forward_weight(kb_ref)
    wa_b, wb_b = backward_weight(ka_ref), backward_weight(kb_ref)
    mix = mix_ref[...]
    mix_t = mix.T

    def fine_windows(dst, middle, rc, rr):
        rows = jnp.concatenate([rr[0:1], middle, rr[3:4]], axis=0)
        left = jnp.concatenate(
            [roll(rr[1:2], 32)] + unpack_column(rc[0], 0) + [roll(rr[4:5], 32)], axis=0
        )
        right = jnp.concatenate(
            [roll(rr[2:3], 96)] + unpack_column(rc[1], 96) + [roll(rr[5:6], 96)], axis=0
        )
        lane = lane_of(rows.shape)
        dst[:, 0:32, :] = jnp.where(
            lane < lo32, left, jnp.where(lane < 32, zero(rows), roll(rows, 32))
        )
        dst[:, 32:64, :] = rows
        dst[:, 64:96, :] = jnp.where(
            lane >= hi96, right, jnp.where(lane >= 96, zero(rows), roll(rows, -32))
        )

    halo_wait(halo_x)
    fine_windows(sfa, x, rcx, rrx)
    conv_rows(sfa, 16, wa_f, 32, lin_a_s)
    lin_a = lin_a_s[...]
    hidden = (lin_a / (1.0 + jnp.exp(-lin_a))).astype(BF).astype(F32).reshape(8, 2, 32, 128)
    coarse = (0.25 * pool_columns(hidden[:, 0] + hidden[:, 1])).astype(BF)

    colc_s[...] = pack_pair(coarse[0:4], coarse[4:8])
    rowc_s[0:1] = pack_pair(coarse[6:7], coarse[7:8])
    rowc_s[1:2] = pack_pair(coarse[0:1], coarse[1:2])
    halo_c = halo_start(2, (colc_s, colc_s), (rowc_s.at[0], rowc_s.at[1]), rcc, rrc)

    halo_wait(halo_f)
    fold_rows = jnp.concatenate([rrf[0:1], fold, rrf[3:4]], axis=0)
    fold_left = jnp.concatenate(
        [roll(rrf[1:2], 64)] + unpack_column(rcf[0], 0) + [roll(rrf[4:5], 64)], axis=0
    )
    fold_right = jnp.concatenate(
        [roll(rrf[2:3], 64)] + unpack_column(rcf[1], 96) + [roll(rrf[5:6], 64)], axis=0
    )
    lane = lane_of(fold_rows.shape)
    fold_wide = jnp.where(
        (lane >= 32) & (lane < 96),
        fold_rows,
        jnp.where(
            lane < lo32, fold_left, jnp.where(lane >= hi96, fold_right, zero(fold_rows))
        ),
    )

    halo_wait(halo_c)
    rows = jnp.concatenate(
        [roll(rrc[0:1], 32), roll(rrc[0:1], -32), coarse, roll(rrc[3:4], 32), roll(rrc[3:4], -32)],
        axis=0,
    )
    left = jnp.concatenate(
        [rrc[1:2], roll(rrc[1:2], 64), rcc[0], roll(rcc[0], 64), rrc[4:5], roll(rrc[4:5], 64)],
        axis=0,
    )
    right = jnp.concatenate(
        [roll(rrc[2:3], 64), rrc[2:3], roll(rcc[1], 64), rcc[1], roll(rrc[5:6], 64), rrc[5:6]],
        axis=0,
    )
    lane = lane_of(rows.shape)
    left = jnp.where(lane < lo64, left, zero(left))
    right = jnp.where(lane >= hi64, right, zero(right))
    scb[:, 0:32, :] = jnp.where(lane < 64, left, roll(rows, 32))
    scb[:, 32:64, :] = jnp.where(
        lane < 32, roll(left, -32), jnp.where(lane < 96, rows, roll(right, 32))
    )
    scb[:, 64:96, :] = jnp.where(lane < 64, roll(rows, -32), right)

    conv_rows(scb, 10, wb_f, 64, lin_b_s)
    lin_b = lin_b_s[...]
    sig_b = sigmoid(lin_b)
    slope_b = sig_b * (1.0 + lin_b * (1.0 - sig_b))
    gated = (lin_b * sig_b)[1:9].astype(BF)
    grad_gated = dot(mix_t, side_by_side([fold_wide[r] for r in range(10)]))
    grad_b = jnp.concatenate(
        [(grad_gated[:, 128 * r : 128 * (r + 1)] * slope_b[r]).astype(BF)[None] for r in range(10)],
        axis=0,
    )
    sgb[:, 0:64, :] = roll(grad_b, 32)
    sgb[:, 64:128, :] = grad_b
    sgb[:, 128:192, :] = roll(grad_b, -32)

    own = grad_b[1:9]
    lane = lane_of(own.shape)
    own = jnp.where((lane >= 32) & (lane < 96), own, zero(own))
    shifts = layer_shifts(own)
    up = side_by_side([jnp.concatenate([s[r] for s in shifts], axis=0) for r in range(8)])
    seen = side_by_side([scb[r + 1 : r + 4].reshape(288, 128) for r in range(8)])
    sum_b = dot_nt(up, seen).astype(BF)
    sum_m = dot_nt(
        side_by_side([fold[r] for r in range(8)]), side_by_side([gated[r] for r in range(8)])
    ).astype(BF)
    n_a, n_b = pa.shape[1], pb.shape[1]

    def put(buf, tile, value):
        n = buf.shape[1]
        buf[tile // n, tile % n] = value

    for i in range(12):
        for l in range(2):
            put(pb, 2 * i + l, sum_b[16 * i : 16 * i + 16, 128 * l : 128 * l + 128])
    rest = side_by_side([sum_b[48 * g : 48 * g + 48, 256:288] for g in range(4)])
    for i in range(3):
        put(pb, 24 + i, rest[16 * i : 16 * i + 16])
    put(pb, 27, side_by_side([sum_m[0:16], sum_m[16:32]]))
    for t in range(B_TILES, g1 * n_b):
        put(pb, t, jnp.zeros((16, 128), BF))

    def spread(buf, dst, ssem, rsem):
        return [
            send(
                buf.at[lax.rem(me1 + i, g1)], dst.at[i - 1],
                ssem.at[0, i], rsem.at[0, i], plane_device(i),
            )
            for i in range(1, g1)
        ]

    spread_b = spread(pb, rb1, b_send, b_recv)

    conv_rows(sgb, 8, wb_b, 32, gc_s)
    grad_coarse = widen_columns(gc_s[...].astype(BF).astype(F32))
    grad_hidden = jnp.concatenate(
        [(ct[:, i] + 0.25 * grad_coarse)[:, None] for i in range(2)], axis=1
    ).reshape(16, 32, 128)
    sig_a = sigmoid(lin_a)
    grad_a = (grad_hidden * (sig_a * (1.0 + lin_a * (1.0 - sig_a)))).astype(BF)
    g_s[...] = grad_a
    colg_s[0] = pack_column(grad_a, 4, 96)
    colg_s[1] = pack_column(grad_a, 4, 0)
    halo_g = halo_start(
        3, (colg_s.at[0], colg_s.at[1]), (g_s.at[15], g_s.at[0]), rcg, rrg
    )

    shifts = layer_shifts(grad_a)
    up = side_by_side([jnp.concatenate([s[r] for s in shifts], axis=0) for r in range(16)])
    seen = side_by_side([sfa[r : r + 3].reshape(288, 128) for r in range(16)])
    sum_a = dot_nt(up, seen).astype(BF)
    for i in range(6):
        for l in range(2):
            put(pa, 2 * i + l, sum_a[16 * i : 16 * i + 16, 128 * l : 128 * l + 128])
    rest = side_by_side([sum_a[32 * g : 32 * g + 32, 256:288] for g in range(3)])
    rest = jnp.concatenate([rest, jnp.zeros((32, 32), BF)], axis=1)
    for i in range(2):
        put(pa, 12 + i, rest[16 * i : 16 * i + 16])
    for t in range(A_TILES, g1 * n_a):
        put(pa, t, jnp.zeros((16, 128), BF))
    spread_a = spread(pa, ra1, a_send, a_recv)

    projected = dot(mix, side_by_side([gated[r] for r in range(8)])).astype(BF).astype(F32)
    projected = jnp.concatenate(
        [projected[:, 128 * r : 128 * (r + 1)][None] for r in range(8)], axis=0
    )
    projected = widen_columns(projected)
    output = jnp.concatenate(
        [(hidden[:, i] + projected)[:, None] for i in range(2)], axis=1
    ).reshape(16, 32, 128)
    out_ref[...] = jnp.transpose(output.astype(BF), (1, 0, 2))

    def cross(copies, buf, arrived, mine, slots, ssem, rsem):
        for copy in copies:
            copy.wait_recv()
        total = buf[me1].astype(F32)
        for i in range(g1 - 1):
            total = total + arrived[i].astype(F32)
        total = total.astype(BF)
        mine[...] = total
        slots[me2] = total
        return [
            send(mine, slots.at[me2], ssem.at[1, i], rsem.at[1, i], line_device(i))
            for i in range(1, g2)
        ]

    def wait_slots(copies, src, slots, count, me, ssem, rsem, stage):
        for i in range(1, count):
            slot = lax.rem(me + count - i, count)
            pltpu.make_async_remote_copy(
                src_ref=src, dst_ref=slots.at[slot], send_sem=ssem.at[stage, i],
                recv_sem=rsem.at[stage, i], device_id=(p, e), device_id_type=MESH,
            ).wait_recv()

    def gather(copies, mine2, slots, mine, result, ssem, rsem):
        wait_slots(copies, mine2, slots, g2, me2, ssem, rsem, 1)
        total = slots[0].astype(F32)
        for i in range(1, g2):
            total = total + slots[i].astype(F32)
        total = total.astype(BF)
        mine[...] = total
        result[me1] = total
        return [
            send(mine, result.at[me1], ssem.at[2, i], rsem.at[2, i], plane_device(i))
            for i in range(1, g1)
        ]

    cross_b = cross(spread_b, pb, rb1, xb2, rb2, b_send, b_recv)
    cross_a = cross(spread_a, pa, ra1, xa2, ra2, a_send, a_recv)

    halo_wait(halo_g)
    fine_windows(sga, grad_a, rcg, rrg)
    conv_rows(sga, 16, wa_b, 32, gi_s)
    gi_ref[...] = jnp.transpose(gi_s[...].astype(BF), (1, 0, 2))

    gather_b = gather(cross_b, xb2, rb2, xb3, resb, b_send, b_recv)
    gather_a = gather(cross_a, xa2, ra2, xa3, resa, a_send, a_recv)

    wait_slots(gather_b, xb3, resb, g1, me1, b_send, b_recv, 2)

    def tile(buf, t):
        n = buf.shape[1]
        return buf[t // n, t % n].astype(F32) * scale

    for c in range(3):
        for l in range(2):
            block = jnp.concatenate([tile(resb, 2 * (4 * c + j) + l) for j in range(4)], axis=0)
            for q in range(4):
                gkb_ref[(4 * l + q) * 3 + c] = block[:, 32 * q : 32 * q + 32]
    rest = jnp.concatenate([tile(resb, 24 + i) for i in range(3)], axis=0)
    rest = jnp.concatenate([rest[:, 32 * g : 32 * g + 32] for g in range(4)], axis=0)
    for c in range(3):
        gkb_ref[24 + c] = rest[64 * c : 64 * c + 64]
    last = tile(resb, 27)
    gm_ref[0:16, :] = last[:, 0:64]
    gm_ref[16:32, :] = last[:, 64:128]

    wait_slots(gather_a, xa3, resa, g1, me1, a_send, a_recv, 2)
    for c in range(3):
        for l in range(2):
            block = jnp.concatenate([tile(resa, 2 * (2 * c + j) + l) for j in range(2)], axis=0)
            for q in range(4):
                gka_ref[(4 * l + q) * 3 + c] = block[:, 32 * q : 32 * q + 32]
    rest = jnp.concatenate([tile(resa, 12 + i) for i in range(2)], axis=0)
    for c in range(3):
        gka_ref[24 + c] = rest[:, 32 * c : 32 * c + 32]

    for copy in pending:
        copy.wait_send()


def shards(n_phi, n_eta, features, cotangent, kernel_a, kernel_b, mixing):
    g1, g2 = 2 * n_eta, n_phi // 2
    n_a, n_b = -(-A_TILES // g1), -(-B_TILES // g1)
    cells = features.shape[1] * features.shape[2] * n_phi * n_eta
    field = jax.ShapeDtypeStruct(features.shape, BF)

    def vm(*shape, dtype=BF):
        return pltpu.VMEM(shape, dtype)

    def sums(n):
        return [
            vm(g1, n, 16, 128), vm(g1 - 1, n, 16, 128), vm(n, 16, 128),
            vm(g2, n, 16, 128), vm(n, 16, 128), vm(g1, n, 16, 128),
        ]

    def halo(n):
        return [vm(2, n, 32, 128), vm(6, 32, 128)]

    dma = pltpu.SemaphoreType.DMA
    wide = max(g1, g2)
    scratch = [
        vm(16, 32, 128), vm(2, 4, 32, 128), *halo(4),
        vm(8, 32, 128), vm(2, 2, 32, 128), *halo(2),
        vm(4, 32, 128), vm(2, 32, 128), *halo(4),
        vm(16, 32, 128), vm(2, 4, 32, 128), *halo(4),
        vm(18, 96, 128), vm(12, 96, 128), vm(10, 192, 128), vm(18, 96, 128),
        vm(16, 32, 128, dtype=F32), vm(10, 64, 128, dtype=F32),
        vm(8, 32, 128, dtype=F32), vm(16, 32, 128, dtype=F32),
        *sums(n_a), *sums(n_b),
        dma((4, 8)), dma((4, 8)),
        dma((3, wide)), dma((3, wide)), dma((3, wide)), dma((3, wide)),
    ]
    vmem = pl.BlockSpec(memory_space=pltpu.VMEM)
    return pl.pallas_call(
        functools.partial(kernel, n_phi, n_eta, 1.0 / math.sqrt(cells)),
        out_shape=(
            field,
            field,
            jax.ShapeDtypeStruct(kernel_a.shape, F32),
            jax.ShapeDtypeStruct(kernel_b.shape, F32),
            jax.ShapeDtypeStruct(mixing.shape, F32),
        ),
        in_specs=[vmem] * 5,
        out_specs=(vmem,) * 5,
        scratch_shapes=scratch,
        compiler_params=pltpu.CompilerParams(collective_id=0, has_side_effects=True),
        name="block_step",
    )(features, cotangent, kernel_a, kernel_b, mixing)


def solution(mesh):
    specs = (P(None, "phi", "eta"), P(None, "phi", "eta"), P(), P(), P())
    body = functools.partial(shards, mesh.shape["phi"], mesh.shape["eta"])
    return jax.shard_map(body, mesh=mesh, in_specs=specs, out_specs=specs, check_vma=False)
```

```python
import functools
import math

import jax
import jax.numpy as jnp
from jax import lax
from jax.experimental import pallas as pl
from jax.experimental.pallas import tpu as pltpu
from jax.sharding import PartitionSpec as P

BF = jnp.bfloat16
F32 = jnp.float32
MESH = pl.DeviceIdType.MESH
DIRS = ((0, 1), (0, -1), (1, 0), (1, 1), (1, -1), (-1, 0), (-1, 1), (-1, -1))
PLANE = 32


def lane_of(shape):
    return lax.broadcasted_iota(jnp.int32, shape, len(shape) - 1)


def roll(x, shift):
    shift %= 128
    return x if shift == 0 else pltpu.roll(x, shift, x.ndim - 1)


def dot(a, b):
    return jnp.dot(a, b, preferred_element_type=F32)


def dot_nt(a, b):
    return lax.dot_general(a, b, (((1,), (1,)), ((), ())), preferred_element_type=F32)


def zero(x):
    return jnp.zeros((), x.dtype)


def side_by_side(rows):
    return jnp.concatenate(rows, axis=1)


def by_quarter(v0, v1, v2, v3):
    lane = lane_of(v0.shape)
    return jnp.where(
        lane < 64, jnp.where(lane < 32, v0, v1), jnp.where(lane < 96, v2, v3)
    )


def pack_column(x, size, start):
    return by_quarter(
        *[roll(x[size * g : size * (g + 1)], 32 * g - start) for g in range(4)]
    )


def unpack_column(packed, want):
    return [roll(packed, want - 32 * g) for g in range(4)]


def pack_pair(x, y):
    return jnp.where(lane_of(x.shape) < 64, roll(x, -32), roll(y, 32))


def widen_columns(x):
    lane = lane_of(x.shape)
    return jnp.where(lane < 32, roll(x, -32), jnp.where(lane < 96, x, roll(x, 32)))


def pool_columns(x):
    lane = lane_of(x.shape)
    both = x + jnp.where(lane < 64, roll(x, 32), roll(x, -32))
    return jnp.where((lane >= 32) & (lane < 96), both, zero(x))


def layer_shifts(x):
    layer = lane_of(x.shape) % 32
    return [
        jnp.where(layer < 31, roll(x, -1), zero(x)),
        x,
        jnp.where(layer > 0, roll(x, 1), zero(x)),
    ]


def conv_rows(src, count, weight, outs, sink):
    layer = lane_of((outs, 128)) % 32
    flat = 3 * src.shape[1]
    for r in range(0, count, 2):
        pair = [src[r + i : r + i + 3].reshape(flat, 128) for i in range(2)]
        z = dot(weight, side_by_side(pair))
        for i in range(2):
            zi = z[:, 128 * i : 128 * (i + 1)]
            low = jnp.where(layer > 0, roll(zi[:outs], 1), 0.0)
            high = jnp.where(layer < 31, roll(zi[2 * outs :], -1), 0.0)
            sink[r + i] = zi[outs : 2 * outs] + low + high


def sigmoid(v):
    return 1.0 / (1.0 + jnp.exp(-v))


def kernel(n_phi, n_eta, scale, *refs):
    ins, (out_ref, gi_ref, gka_ref, gkb_ref, gm_ref) = refs[:5], refs[5:10]
    (
        f_ref, ct_ref, ka_ref, kb_ref, mix_ref, load_sem,
        x_s, colx_s, rx,
        fold_s, colf_s, rf,
        colc_s, rowc_s, rc,
        g_s, colg_s, rg,
        sfa, scb, sgb, sga, slope_a_s, lin_a_s, lin_b_s, gc_s, gi_s,
        pa, ra, pb, rb, x2, r2, x3, res,
        h_send, h_recv, s_send, s_recv,
    ) = refs[10:]
    p = lax.axis_index("phi")
    e = lax.axis_index("eta")
    g1, g2 = 4 * n_eta, n_phi // 4
    me1 = lax.rem(p, 4) * n_eta + e
    me2 = p // 4

    def wrap(i, n):
        return jnp.where(i >= n, i - n, i)

    def halo_device(d):
        return (wrap(p + d[0] % n_phi, n_phi), wrap(e + d[1] % n_eta, n_eta))

    def plane_device(i):
        q = wrap(me1 + i, g1)
        return (me2 * 4 + q // n_eta, lax.rem(q, n_eta))

    def line_device(i):
        r = wrap(me2 + i, g2)
        return (r * 4 + lax.rem(p, 4), e)

    barrier = pltpu.get_barrier_semaphore()
    targets = [line_device(i) for i in sorted(range(1, g2), key=lambda i: -min(i, g2 - i))]
    targets += [plane_device(i) for i in range(1, g1)]
    targets += [halo_device(d) for d in DIRS]
    for target in targets:
        pl.semaphore_signal(barrier, inc=1, device_id=target, device_id_type=MESH)

    loads = [
        pltpu.make_async_copy(src, dst, load_sem.at[k])
        for k, (src, dst) in enumerate(zip(ins, (f_ref, ct_ref, ka_ref, kb_ref, mix_ref)))
    ]
    for load in loads:
        load.start()

    departures = []

    def send(src, dst, ssem, rsem, target):
        pltpu.make_async_remote_copy(
            src_ref=src, dst_ref=dst, send_sem=ssem, recv_sem=rsem,
            device_id=target, device_id_type=MESH,
        ).start()

    def whole(ref, ssem, rsem):
        return pltpu.make_async_remote_copy(
            src_ref=ref, dst_ref=ref, send_sem=ssem, recv_sem=rsem,
            device_id=(p, e), device_id_type=MESH,
        )

    def halo_start(which, cols, rows, arrived):
        n = (arrived.shape[0] - 6) // 2
        ssem, rsem = h_send.at[which], h_recv.at[which]
        for k, d in enumerate(DIRS):
            if k < 2:
                src, dst = cols[k], arrived.at[pl.ds(n * k, n)]
            else:
                src, dst = rows[0 if d[0] > 0 else 1], arrived.at[2 * n + k - 2]
            send(src, dst, ssem, rsem, halo_device(d))
        copy = whole(arrived, ssem, rsem)
        departures.append(copy)
        return copy

    def halo_parts(arrived):
        n = (arrived.shape[0] - 6) // 2
        rows = [arrived[2 * n + j : 2 * n + j + 1] for j in range(6)]
        return (arrived[0:n], arrived[n : 2 * n]), rows

    has_left = e > 0
    has_right = e < n_eta - 1
    lo32 = jnp.where(has_left, 32, 0)
    lo64 = jnp.where(has_left, 64, 0)
    hi96 = jnp.where(has_right, 96, 128)
    hi64 = jnp.where(has_right, 64, 128)

    loads[0].wait()
    x = jnp.transpose(f_ref[...], (1, 0, 2))
    x_s[...] = x
    colx_s[0] = pack_column(x, 4, 96)
    colx_s[1] = pack_column(x, 4, 0)
    pl.semaphore_wait(barrier, len(targets))
    halo_x = halo_start(
        0, (colx_s.at[0], colx_s.at[1]), (x_s.at[15], x_s.at[0]), rx
    )

    for load in loads[1:]:
        load.wait()
    ct = jnp.transpose(ct_ref[...], (1, 0, 2)).astype(F32).reshape(8, 2, 32, 128)
    fold = pool_columns(ct[:, 0] + ct[:, 1]).astype(BF)
    fold_s[...] = fold
    colf_s[0] = pack_column(fold, 2, 64)
    colf_s[1] = pack_column(fold, 2, 32)
    halo_f = halo_start(
        1, (colf_s.at[0], colf_s.at[1]), (fold_s.at[7], fold_s.at[0]), rf
    )

    def forward_weight(ref):
        return jnp.concatenate(
            [side_by_side([ref[3 * ab + c] for ab in range(9)]) for c in range(3)], axis=0
        )

    def backward_weight(ref):
        return jnp.concatenate(
            [side_by_side([ref[26 - 3 * ab - c] for c in range(3)]) for ab in range(9)], axis=0
        ).T

    wa_f, wa_b = forward_weight(ka_ref), backward_weight(ka_ref)
    wb_f = jnp.concatenate(
        [side_by_side([kb_ref[3 * ab + c] for c in range(3)]) for ab in range(9)], axis=0
    ).T
    wb_b = jnp.concatenate(
        [side_by_side([kb_ref[26 - 3 * ab - c] for ab in range(9)]) for c in range(3)], axis=0
    )
    mix = mix_ref[...]
    mix_t = mix.T

    def fine_windows(dst, middle, arrived):
        cols, rim = halo_parts(arrived)
        rows = jnp.concatenate([rim[0], middle, rim[3]], axis=0)
        left = jnp.concatenate(
            [roll(rim[1], 32)] + unpack_column(cols[0], 0) + [roll(rim[4], 32)], axis=0
        )
        right = jnp.concatenate(
            [roll(rim[2], 96)] + unpack_column(cols[1], 96) + [roll(rim[5], 96)], axis=0
        )
        lane = lane_of(rows.shape)
        dst[:, 0:32, :] = jnp.where(
            lane < lo32, left, jnp.where(lane < 32, zero(rows), roll(rows, 32))
        )
        dst[:, 32:64, :] = rows
        dst[:, 64:96, :] = jnp.where(
            lane >= hi96, right, jnp.where(lane >= 96, zero(rows), roll(rows, -32))
        )

    halo_x.wait_recv()
    fine_windows(sfa, x, rx)
    conv_rows(sfa, 16, wa_f, 32, lin_a_s)
    lin_a = lin_a_s[...]
    hidden = (lin_a / (1.0 + jnp.exp(-lin_a))).astype(BF).astype(F32).reshape(8, 2, 32, 128)
    coarse = (0.25 * pool_columns(hidden[:, 0] + hidden[:, 1])).astype(BF)

    colc_s[...] = pack_pair(coarse[0:4], coarse[4:8])
    rowc_s[0:1] = pack_pair(coarse[6:7], coarse[7:8])
    rowc_s[1:2] = pack_pair(coarse[0:1], coarse[1:2])
    halo_c = halo_start(2, (colc_s, colc_s), (rowc_s.at[0], rowc_s.at[1]), rc)

    halo_f.wait_recv()
    cols, rim = halo_parts(rf)
    fold_rows = jnp.concatenate([rim[0], fold, rim[3]], axis=0)
    fold_left = jnp.concatenate(
        [roll(rim[1], 64)] + unpack_column(cols[0], 0) + [roll(rim[4], 64)], axis=0
    )
    fold_right = jnp.concatenate(
        [roll(rim[2], 64)] + unpack_column(cols[1], 96) + [roll(rim[5], 64)], axis=0
    )
    lane = lane_of(fold_rows.shape)
    fold_wide = jnp.where(
        (lane >= 32) & (lane < 96),
        fold_rows,
        jnp.where(
            lane < lo32, fold_left, jnp.where(lane >= hi96, fold_right, zero(fold_rows))
        ),
    )

    grad_gated = dot(mix_t, side_by_side([fold_wide[r] for r in range(10)]))
    sig_a = sigmoid(lin_a)
    slope_a_s[...] = sig_a * (1.0 + lin_a * (1.0 - sig_a))

    halo_c.wait_recv()
    cols, rim = halo_parts(rc)
    rows = jnp.concatenate(
        [roll(rim[0], 32), roll(rim[0], -32), coarse, roll(rim[3], 32), roll(rim[3], -32)],
        axis=0,
    )
    left = jnp.concatenate(
        [rim[1], roll(rim[1], 64), cols[0], roll(cols[0], 64), rim[4], roll(rim[4], 64)],
        axis=0,
    )
    right = jnp.concatenate(
        [roll(rim[2], 64), rim[2], roll(cols[1], 64), cols[1], roll(rim[5], 64), rim[5]],
        axis=0,
    )
    lane = lane_of(rows.shape)
    left = jnp.where(lane < lo64, left, zero(left))
    right = jnp.where(lane >= hi64, right, zero(right))
    scb[:, 0:32, :] = jnp.where(lane < 64, left, roll(rows, 32))
    scb[:, 32:64, :] = jnp.where(
        lane < 32, roll(left, -32), jnp.where(lane < 96, rows, roll(right, 32))
    )
    scb[:, 64:96, :] = jnp.where(lane < 64, roll(rows, -32), right)

    conv_rows(scb, 10, wb_f, 64, lin_b_s)
    lin_b = lin_b_s[...]
    sig_b = sigmoid(lin_b)
    slope_b = sig_b * (1.0 + lin_b * (1.0 - sig_b))
    gated = (lin_b * sig_b)[1:9].astype(BF)
    grad_b = jnp.concatenate(
        [(grad_gated[:, 128 * r : 128 * (r + 1)] * slope_b[r]).astype(BF)[None] for r in range(10)],
        axis=0,
    )
    sgb[:, 0:64, :] = roll(grad_b, 32)
    sgb[:, 64:128, :] = grad_b
    sgb[:, 128:192, :] = roll(grad_b, -32)

    own = grad_b[1:9]
    lane = lane_of(own.shape)
    own = jnp.where((lane >= 32) & (lane < 96), own, zero(own))
    shifts = layer_shifts(own)
    up = side_by_side([jnp.concatenate([s[r] for s in shifts], axis=0) for r in range(8)])
    seen = side_by_side([scb[r + 1 : r + 4].reshape(288, 128) for r in range(8)])
    sum_b = dot_nt(seen, up)
    sum_m = dot_nt(
        side_by_side([fold[r] for r in range(8)]), side_by_side([gated[r] for r in range(8)])
    )
    for i in range(18):
        pb[i] = sum_b[16 * i : 16 * i + 16, 0:128].astype(BF)
    rest = side_by_side([sum_b[144 * g : 144 * g + 144, 128:192] for g in range(2)])
    for i in range(9):
        pb[18 + i] = rest[16 * i : 16 * i + 16].astype(BF)
    pb[27] = side_by_side([sum_m[0:16], sum_m[16:32]]).astype(BF)
    for t in range(28, PLANE):
        pb[t] = jnp.zeros((16, 128), BF)

    def spread(buf, dst, k):
        for i in range(1, g1):
            q = wrap(me1 + i, g1)
            send(buf.at[q], dst.at[i - 1], s_send.at[k], s_recv.at[k], plane_device(i))
        copy = whole(dst, s_send.at[k], s_recv.at[k])
        departures.append(copy)
        return copy

    spread_b = spread(pb, rb, 0)

    conv_rows(sgb, 8, wb_b, 32, gc_s)
    grad_coarse = widen_columns(gc_s[...].astype(BF).astype(F32))
    grad_hidden = jnp.concatenate(
        [(ct[:, i] + 0.25 * grad_coarse)[:, None] for i in range(2)], axis=1
    ).reshape(16, 32, 128)
    grad_a = (grad_hidden * slope_a_s[...]).astype(BF)
    g_s[...] = grad_a
    colg_s[0] = pack_column(grad_a, 4, 96)
    colg_s[1] = pack_column(grad_a, 4, 0)
    shifts = layer_shifts(grad_a)
    up = side_by_side([jnp.concatenate([s[r] for s in shifts], axis=0) for r in range(16)])
    seen = side_by_side([sfa[r : r + 3].reshape(288, 128) for r in range(16)])
    sum_a = dot_nt(up, seen)
    for i in range(12):
        for l in range(2):
            pa[2 * i + l] = sum_a[8 * i : 8 * i + 8, 128 * l : 128 * l + 128].astype(BF)
    rest = side_by_side([sum_a[32 * g : 32 * g + 32, 256:288] for g in range(3)])
    rest = jnp.concatenate([rest, jnp.zeros((32, 32), F32)], axis=1)
    for i in range(4):
        pa[24 + i] = rest[8 * i : 8 * i + 8].astype(BF)
    for t in range(28, PLANE):
        pa[t] = jnp.zeros((8, 128), BF)
    spread_a = spread(pa, ra, 1)
    projected = dot(mix, side_by_side([gated[r] for r in range(8)])).astype(BF).astype(F32)
    projected = jnp.concatenate(
        [projected[:, 128 * r : 128 * (r + 1)][None] for r in range(8)], axis=0
    )
    projected = widen_columns(projected)
    output = jnp.concatenate(
        [(hidden[:, i] + projected)[:, None] for i in range(2)], axis=1
    ).reshape(16, 32, 128)
    out_ref[...] = jnp.transpose(output.astype(BF), (1, 0, 2))

    spread_b.wait_recv()
    total_b = pb[me1].astype(F32)
    for i in range(g1 - 1):
        total_b = total_b + rb[i].astype(F32)
    spread_a.wait_recv()
    total_a = pa[me1].astype(F32)
    for i in range(g1 - 1):
        total_a = total_a + ra[i].astype(F32)
    total = jnp.concatenate([total_b, total_a], axis=0).astype(BF)
    x2[...] = total
    r2[me2] = total
    for i in range(1, g2):
        send(x2, r2.at[me2], s_send.at[2], s_recv.at[2], line_device(i))
    crossed = whole(r2.at[pl.ds(0, g2 - 1)], s_send.at[2], s_recv.at[2])
    departures.append(crossed)

    halo_g = halo_start(
        3, (colg_s.at[0], colg_s.at[1]), (g_s.at[15], g_s.at[0]), rg
    )

    crossed.wait_recv()
    total = r2[0].astype(F32)
    for i in range(1, g2):
        total = total + r2[i].astype(F32)
    total = total.astype(BF)
    x3[...] = total
    res[me1] = total
    for i in range(1, g1):
        send(x3, res.at[me1], s_send.at[3], s_recv.at[3], plane_device(i))
    gathered = whole(res.at[pl.ds(0, g1 - 1)], s_send.at[3], s_recv.at[3])
    departures.append(gathered)
    halo_g.wait_recv()
    fine_windows(sga, grad_a, rg)
    conv_rows(sga, 16, wa_b, 32, gi_s)
    gi_ref[...] = jnp.transpose(gi_s[...].astype(BF), (1, 0, 2))

    gathered.wait_recv()

    for ab in range(9):
        for h in range(2):
            rows = slice(16 * h, 16 * h + 16)
            u = 2 * ab + h
            pair = res[u, 0:16].astype(F32) * scale
            gkb_ref[3 * ab, rows, :] = pair[:, 0:64]
            gkb_ref[3 * ab + 1, rows, :] = pair[:, 64:128]
            g = u // 9
            rest = res[18 + u % 9, 0:16].astype(F32) * scale
            gkb_ref[3 * ab + 2, rows, :] = rest[:, 64 * g : 64 * g + 64]
    last = res[27, 0:16].astype(F32) * scale
    gm_ref[0:16, :] = last[:, 0:64]
    gm_ref[16:32, :] = last[:, 64:128]

    for c in range(3):
        for h in range(4):
            rows = slice(8 * h, 8 * h + 8)
            for l in range(2):
                block = res[2 * (4 * c + h) + l, 16:24].astype(F32) * scale
                for q in range(4):
                    gka_ref[(4 * l + q) * 3 + c, rows, :] = block[:, 32 * q : 32 * q + 32]
            rest = res[24 + h, 16:24].astype(F32) * scale
            gka_ref[24 + c, rows, :] = rest[:, 32 * c : 32 * c + 32]

    for copy in departures:
        copy.wait_send()


def writer(*refs):
    sems = refs[10]
    copies = [
        pltpu.make_async_copy(src, dst, sems.at[k])
        for k, (src, dst) in enumerate(zip(refs[:5], refs[5:10]))
    ]
    for copy in copies:
        copy.start()
    for copy in copies:
        copy.wait()


def shards(n_phi, n_eta, features, cotangent, kernel_a, kernel_b, mixing):
    g1, g2 = 4 * n_eta, n_phi // 4
    assert g1 == PLANE
    cells = features.shape[1] * features.shape[2] * n_phi * n_eta
    kernel_b = jnp.swapaxes(kernel_b, 1, 2)
    ins = (features, cotangent, kernel_a, kernel_b, mixing)
    types = (BF, BF, F32, F32, F32)

    def vm(*shape, dtype=BF):
        return pltpu.VMEM(shape, dtype)

    def halo(n):
        return [vm(2 * n + 6, 32, 128)]

    dma = pltpu.SemaphoreType.DMA
    scratch = [
        *[vm(*a.shape) for a in ins], dma((5,)),
        vm(16, 32, 128), vm(2, 4, 32, 128), *halo(4),
        vm(8, 32, 128), vm(2, 2, 32, 128), *halo(2),
        vm(4, 32, 128), vm(2, 32, 128), *halo(4),
        vm(16, 32, 128), vm(2, 4, 32, 128), *halo(4),
        vm(18, 96, 128), vm(12, 96, 128), vm(10, 192, 128), vm(18, 96, 128),
        vm(16, 32, 128, dtype=F32), vm(16, 32, 128, dtype=F32), vm(10, 64, 128, dtype=F32),
        vm(8, 32, 128, dtype=F32), vm(16, 32, 128, dtype=F32),
        vm(g1, 8, 128), vm(g1 - 1, 8, 128), vm(g1, 16, 128), vm(g1 - 1, 16, 128),
        vm(24, 128), vm(g2, 24, 128), vm(24, 128), vm(g1, 24, 128),
        *[dma((4,)) for _ in range(4)],
    ]
    vmem = pl.BlockSpec(memory_space=pltpu.VMEM)
    anywhere = pl.BlockSpec(memory_space=pl.ANY)
    shapes = [a.shape for a in ins]
    outs = pl.pallas_call(
        functools.partial(kernel, n_phi, n_eta, 1.0 / math.sqrt(cells)),
        out_shape=tuple(pltpu.VMEM(s, t) for s, t in zip(shapes, types)),
        in_specs=[anywhere] * 5,
        out_specs=(vmem,) * 5,
        scratch_shapes=scratch,
        compiler_params=pltpu.CompilerParams(collective_id=0, has_side_effects=True),
        name="block_step",
    )(*ins)
    outs = pl.pallas_call(
        writer,
        out_shape=tuple(jax.ShapeDtypeStruct(s, t) for s, t in zip(shapes, types)),
        in_specs=[vmem] * 5,
        out_specs=(anywhere,) * 5,
        scratch_shapes=[dma((5,))],
        name="write_out",
    )(*[pltpu.with_memory_space_constraint(o, pltpu.VMEM) for o in outs])
    return (*outs[:3], jnp.swapaxes(outs[3], 1, 2), outs[4])


def solution(mesh):
    specs = (P(None, "phi", "eta"), P(None, "phi", "eta"), P(), P(), P())
    body = functools.partial(shards, mesh.shape["phi"], mesh.shape["eta"])
    return jax.shard_map(body, mesh=mesh, in_specs=specs, out_specs=specs, check_vma=False)
```

```python
import functools
import math

import jax
import jax.numpy as jnp
from jax import lax
from jax.experimental import pallas as pl
from jax.experimental.pallas import tpu as pltpu
from jax.sharding import PartitionSpec as P

BF = jnp.bfloat16
F32 = jnp.float32
MESH = pl.DeviceIdType.MESH
DIRS = ((0, 1), (0, -1), (1, 0), (1, 1), (1, -1), (-1, 0), (-1, 1), (-1, -1))
PLANE = 32


def lane_of(shape):
    return lax.broadcasted_iota(jnp.int32, shape, len(shape) - 1)


def roll(x, shift):
    shift %= 128
    return x if shift == 0 else pltpu.roll(x, shift, x.ndim - 1)


def dot(a, b):
    return jnp.dot(a, b, preferred_element_type=F32)


def dot_nt(a, b):
    return lax.dot_general(a, b, (((1,), (1,)), ((), ())), preferred_element_type=F32)


def zero(x):
    return jnp.zeros((), x.dtype)


def side_by_side(rows):
    return jnp.concatenate(rows, axis=1)


def by_quarter(v0, v1, v2, v3):
    lane = lane_of(v0.shape)
    return jnp.where(
        lane < 64, jnp.where(lane < 32, v0, v1), jnp.where(lane < 96, v2, v3)
    )


def pack_column(x, size, start):
    return by_quarter(
        *[roll(x[size * g : size * (g + 1)], 32 * g - start) for g in range(4)]
    )


def unpack_column(packed, want):
    return [roll(packed, want - 32 * g) for g in range(4)]


def pack_pair(x, y):
    return jnp.where(lane_of(x.shape) < 64, roll(x, -32), roll(y, 32))


def widen_pairs(x):
    up, down, across = roll(x, 32), roll(x, -32), roll(x, 64)
    low, high = by_quarter(x, up, up, across), by_quarter(across, down, down, x)
    return jnp.concatenate([low, high], axis=0)


def pool_columns(x):
    lane = lane_of(x.shape)
    both = x + jnp.where(lane < 64, roll(x, 32), roll(x, -32))
    return jnp.where((lane >= 32) & (lane < 96), both, zero(x))


def layer_shifts(x):
    layer = lane_of(x.shape) % 32
    return [
        jnp.where(layer < 31, roll(x, -1), zero(x)),
        x,
        jnp.where(layer > 0, roll(x, 1), zero(x)),
    ]


def conv_rows(src, count, weight, outs, sink):
    layer = lane_of((outs, 128)) % 32
    flat = 3 * src.shape[1]
    for r in range(0, count, 2):
        pair = [src[r + i : r + i + 3].reshape(flat, 128) for i in range(2)]
        z = dot(weight, side_by_side(pair))
        for i in range(2):
            zi = z[:, 128 * i : 128 * (i + 1)]
            low = jnp.where(layer > 0, roll(zi[:outs], 1), 0.0)
            high = jnp.where(layer < 31, roll(zi[2 * outs :], -1), 0.0)
            sink[r + i] = zi[outs : 2 * outs] + low + high


def sigmoid(v):
    return 1.0 / (1.0 + jnp.exp(-v))


def kernel(n_phi, n_eta, scale, *refs):
    ins, (out_ref, gi_ref, gka_ref, gkb_ref, gm_ref) = refs[:5], refs[5:10]
    (
        f_ref, ct_ref, ka_ref, kb_ref, mix_ref, load_sem,
        x_s, colx_s, rx,
        fold_s, colf_s, rf,
        colc_s, rowc_s, rc,
        g_s, colg_s, rg,
        sfa, sft, scb, sgb, sga, slope_a_s, lin_a_s, lin_b_s, gc_s, gi_s,
        pa, ra, xa2, ra2, xa3, resa, pb, rb, xb2, rb2, xb3, resb,
        h_send, h_recv, s_send, s_recv,
    ) = refs[10:]
    p = lax.axis_index("phi")
    e = lax.axis_index("eta")
    g1, g2 = 4 * n_eta, n_phi // 4
    me1 = lax.rem(p, 4) * n_eta + e
    me2 = p // 4

    def wrap(i, n):
        return jnp.where(i >= n, i - n, i)

    def halo_device(d):
        return (wrap(p + d[0] % n_phi, n_phi), wrap(e + d[1] % n_eta, n_eta))

    def plane_device(i):
        q = wrap(me1 + i, g1)
        return (me2 * 4 + q // n_eta, lax.rem(q, n_eta))

    def line_device(i):
        r = wrap(me2 + i, g2)
        return (r * 4 + lax.rem(p, 4), e)

    barrier = pltpu.get_barrier_semaphore()
    targets = [halo_device(d) for d in DIRS]
    targets += [line_device(i) for i in sorted(range(1, g2), key=lambda i: -min(i, g2 - i))]
    targets += [plane_device(i) for i in range(1, g1)]
    for target in targets:
        pl.semaphore_signal(barrier, inc=1, device_id=target, device_id_type=MESH)

    loads = [
        pltpu.make_async_copy(src, dst, load_sem.at[k])
        for k, (src, dst) in enumerate(zip(ins, (f_ref, ct_ref, ka_ref, kb_ref, mix_ref)))
    ]
    for load in loads:
        load.start()

    departures = []

    def send(src, dst, ssem, rsem, target):
        pltpu.make_async_remote_copy(
            src_ref=src, dst_ref=dst, send_sem=ssem, recv_sem=rsem,
            device_id=target, device_id_type=MESH,
        ).start()

    def whole(ref, ssem, rsem):
        return pltpu.make_async_remote_copy(
            src_ref=ref, dst_ref=ref, send_sem=ssem, recv_sem=rsem,
            device_id=(p, e), device_id_type=MESH,
        )

    def halo_start(which, cols, rows, arrived):
        n = (arrived.shape[0] - 6) // 2
        ssem, rsem = h_send.at[which], h_recv.at[which]
        for k, d in sorted(enumerate(DIRS), key=lambda kd: -abs(kd[1][0]) - abs(kd[1][1])):
            if k < 2:
                src, dst = cols[k], arrived.at[pl.ds(n * k, n)]
            else:
                src, dst = rows[0 if d[0] > 0 else 1], arrived.at[2 * n + k - 2]
            send(src, dst, ssem, rsem, halo_device(d))
        copy = whole(arrived, ssem, rsem)
        departures.append(copy)
        return copy

    def halo_parts(arrived):
        n = (arrived.shape[0] - 6) // 2
        rows = [arrived[2 * n + j : 2 * n + j + 1] for j in range(6)]
        return (arrived[0:n], arrived[n : 2 * n]), rows

    has_left = e > 0
    has_right = e < n_eta - 1
    lo32 = jnp.where(has_left, 32, 0)
    lo64 = jnp.where(has_left, 64, 0)
    hi96 = jnp.where(has_right, 96, 128)
    hi64 = jnp.where(has_right, 64, 128)

    loads[0].wait()
    x = jnp.transpose(f_ref[...], (1, 0, 2))
    x_s[...] = x
    colx_s[0] = pack_column(x, 4, 96)
    colx_s[1] = pack_column(x, 4, 0)
    pl.semaphore_wait(barrier, len(targets))
    halo_x = halo_start(
        0, (colx_s.at[0], colx_s.at[1]), (x_s.at[15], x_s.at[0]), rx
    )

    for load in loads[1:]:
        load.wait()
    ct = jnp.transpose(ct_ref[...], (1, 0, 2)).astype(F32).reshape(8, 2, 32, 128)
    fold = pool_columns(ct[:, 0] + ct[:, 1]).astype(BF)
    fold_s[...] = fold
    colf_s[0] = pack_column(fold, 2, 64)
    colf_s[1] = pack_column(fold, 2, 32)
    halo_f = halo_start(
        1, (colf_s.at[0], colf_s.at[1]), (fold_s.at[7], fold_s.at[0]), rf
    )

    def forward_weight(ref):
        return jnp.concatenate(
            [side_by_side([ref[3 * ab + c] for ab in range(9)]) for c in range(3)], axis=0
        )

    def backward_weight(ref):
        return jnp.concatenate(
            [side_by_side([ref[26 - 3 * ab - c] for c in range(3)]) for ab in range(9)], axis=0
        ).T

    wa_f, wa_b = forward_weight(ka_ref), backward_weight(ka_ref)
    wb_f = jnp.concatenate(
        [side_by_side([kb_ref[3 * ab + c] for c in range(3)]) for ab in range(9)], axis=0
    ).T
    wb_b = jnp.concatenate(
        [side_by_side([kb_ref[26 - 3 * ab - c] for ab in range(9)]) for c in range(3)], axis=0
    )
    mix = mix_ref[...]
    mix_t = mix.T

    def fine_windows_own(dst, rows):
        lane = lane_of(rows.shape)
        dst[1:17, 0:32, :] = jnp.where(lane < 32, zero(rows), roll(rows, 32))
        dst[1:17, 32:64, :] = rows
        dst[1:17, 64:96, :] = jnp.where(lane >= 96, zero(rows), roll(rows, -32))

    def fine_windows_rim(dst, arrived):
        cols, rim = halo_parts(arrived)
        lane = lane_of((16, 32, 128))
        left = jnp.concatenate(unpack_column(cols[0], 0), axis=0)
        right = jnp.concatenate(unpack_column(cols[1], 96), axis=0)
        dst[1:17, 0:32, :] = jnp.where(lane < lo32, left, dst[1:17, 0:32, :])
        dst[1:17, 64:96, :] = jnp.where(lane >= hi96, right, dst[1:17, 64:96, :])
        lane = lane_of((1, 32, 128))
        for k, at in ((0, 0), (3, 17)):
            rows, left, right = rim[k], roll(rim[k + 1], 32), roll(rim[k + 2], 96)
            dst[at : at + 1, 0:32, :] = jnp.where(
                lane < lo32, left, jnp.where(lane < 32, zero(rows), roll(rows, 32))
            )
            dst[at : at + 1, 32:64, :] = rows
            dst[at : at + 1, 64:96, :] = jnp.where(
                lane >= hi96, right, jnp.where(lane >= 96, zero(rows), roll(rows, -32))
            )

    fine_windows_own(sfa, x)

    halo_x.wait_recv()
    fine_windows_rim(sfa, rx)
    conv_rows(sfa, 16, wa_f, 32, lin_a_s)
    lin_a = lin_a_s[...]
    hidden = (lin_a / (1.0 + jnp.exp(-lin_a))).astype(BF).astype(F32).reshape(8, 2, 32, 128)
    coarse = (0.25 * pool_columns(hidden[:, 0] + hidden[:, 1])).astype(BF)

    colc_s[...] = pack_pair(coarse[0:4], coarse[4:8])
    rowc_s[0:1] = pack_pair(coarse[6:7], coarse[7:8])
    rowc_s[1:2] = pack_pair(coarse[0:1], coarse[1:2])
    halo_c = halo_start(2, (colc_s, colc_s), (rowc_s.at[0], rowc_s.at[1]), rc)

    halo_f.wait_recv()
    cols, rim = halo_parts(rf)
    fold_rows = jnp.concatenate([rim[0], fold, rim[3]], axis=0)
    fold_left = jnp.concatenate(
        [roll(rim[1], 64)] + unpack_column(cols[0], 0) + [roll(rim[4], 64)], axis=0
    )
    fold_right = jnp.concatenate(
        [roll(rim[2], 64)] + unpack_column(cols[1], 96) + [roll(rim[5], 64)], axis=0
    )
    lane = lane_of(fold_rows.shape)
    fold_wide = jnp.where(
        (lane >= 32) & (lane < 96),
        fold_rows,
        jnp.where(
            lane < lo32, fold_left, jnp.where(lane >= hi96, fold_right, zero(fold_rows))
        ),
    )

    fold_pairs = pack_pair(fold[0:4], fold[4:8])
    grad_gated = dot(mix_t, side_by_side([fold_wide[r] for r in range(10)]))
    sig_a = sigmoid(lin_a)
    slope_a_s[...] = sig_a * (1.0 + lin_a * (1.0 - sig_a))

    own_rows = slice(2, 10)
    lane = lane_of(coarse.shape)
    scb[own_rows, 0:32, :] = jnp.where(lane < 64, zero(coarse), roll(coarse, 32))
    scb[own_rows, 32:64, :] = coarse
    scb[own_rows, 64:96, :] = jnp.where(lane < 64, roll(coarse, -32), zero(coarse))

    for r in range(16):
        sft[r] = sfa[r : r + 3].reshape(288, 128).T

    halo_c.wait_recv()
    cols, rim = halo_parts(rc)

    def two(*parts):
        return jnp.concatenate(parts, axis=0)

    left, right = two(cols[0], roll(cols[0], 64)), two(roll(cols[1], 64), cols[1])
    left = jnp.where(lane < lo64, left, zero(left))
    right = jnp.where(lane >= hi64, right, zero(right))
    scb[own_rows, 0:32, :] = jnp.where(lane < 64, left, scb[own_rows, 0:32, :])
    scb[own_rows, 32:64, :] = jnp.where(
        lane < 32, roll(left, -32), jnp.where(lane < 96, coarse, roll(right, 32))
    )
    scb[own_rows, 64:96, :] = jnp.where(lane < 64, scb[own_rows, 64:96, :], right)
    lane = lane_of((2, 32, 128))
    for k, at in ((0, 0), (3, 10)):
        rows = two(roll(rim[k], 32), roll(rim[k], -32))
        left, right = two(rim[k + 1], roll(rim[k + 1], 64)), two(roll(rim[k + 2], 64), rim[k + 2])
        left = jnp.where(lane < lo64, left, zero(left))
        right = jnp.where(lane >= hi64, right, zero(right))
        scb[at : at + 2, 0:32, :] = jnp.where(lane < 64, left, roll(rows, 32))
        scb[at : at + 2, 32:64, :] = jnp.where(
            lane < 32, roll(left, -32), jnp.where(lane < 96, rows, roll(right, 32))
        )
        scb[at : at + 2, 64:96, :] = jnp.where(lane < 64, roll(rows, -32), right)

    conv_rows(scb, 10, wb_f, 64, lin_b_s)
    lin_b = lin_b_s[...]
    sig_b = sigmoid(lin_b)
    slope_b = sig_b * (1.0 + lin_b * (1.0 - sig_b))
    gated = (lin_b * sig_b)[1:9].astype(BF)
    grad_b = jnp.concatenate(
        [(grad_gated[:, 128 * r : 128 * (r + 1)] * slope_b[r]).astype(BF)[None] for r in range(10)],
        axis=0,
    )
    top, low = grad_b[0:6], grad_b[4:10]
    lane = lane_of(top.shape)
    sgb[:, 0:64, :] = jnp.where(lane < 64, top, roll(low, 64))
    sgb[:, 64:128, :] = pack_pair(top, low)
    sgb[:, 128:192, :] = jnp.where(lane < 64, roll(top, 64), low)

    shifts = layer_shifts(sgb[1:5, 64:128, :])
    up = side_by_side([jnp.concatenate([s[r] for s in shifts], axis=0) for r in range(4)])
    seen = pack_pair(scb[1:7], scb[5:11])
    seen = side_by_side([seen[r : r + 3].reshape(288, 128) for r in range(4)])
    gated = pack_pair(gated[0:4], gated[4:8])
    sum_b = dot_nt(seen, up)
    sum_m = dot_nt(
        side_by_side([fold_pairs[r] for r in range(4)]), side_by_side([gated[r] for r in range(4)])
    )
    for i in range(18):
        pb[i] = sum_b[16 * i : 16 * i + 16, 0:128].astype(BF)
    rest = side_by_side([sum_b[144 * g : 144 * g + 144, 128:192] for g in range(2)])
    for i in range(9):
        pb[18 + i] = rest[16 * i : 16 * i + 16].astype(BF)
    pb[27] = side_by_side([sum_m[0:16], sum_m[16:32]]).astype(BF)
    for t in range(28, PLANE):
        pb[t] = jnp.zeros((16, 128), BF)

    def spread(buf, dst, k):
        for i in range(1, g1):
            q = wrap(me1 + i, g1)
            send(buf.at[q], dst.at[i - 1], s_send.at[k], s_recv.at[k], plane_device(i))
        copy = whole(dst, s_send.at[k], s_recv.at[k])
        departures.append(copy)
        return copy

    spread_b = spread(pb, rb, 0)

    conv_rows(sgb, 4, wb_b, 32, gc_s)
    grad_coarse = widen_pairs(gc_s[...].astype(BF).astype(F32))
    grad_hidden = jnp.concatenate(
        [(ct[:, i] + 0.25 * grad_coarse)[:, None] for i in range(2)], axis=1
    ).reshape(16, 32, 128)
    grad_a = (grad_hidden * slope_a_s[...]).astype(BF)
    g_s[...] = grad_a
    shifts = layer_shifts(grad_a)
    up = side_by_side([jnp.concatenate([s[r] for s in shifts], axis=0) for r in range(16)])
    sum_a = dot(up, sft[...].reshape(2048, 288))
    for i in range(12):
        for l in range(2):
            pa[2 * i + l] = sum_a[8 * i : 8 * i + 8, 128 * l : 128 * l + 128].astype(BF)
    rest = side_by_side([sum_a[32 * g : 32 * g + 32, 256:288] for g in range(3)])
    rest = jnp.concatenate([rest, jnp.zeros((32, 32), F32)], axis=1)
    for i in range(4):
        pa[24 + i] = rest[8 * i : 8 * i + 8].astype(BF)
    for t in range(28, PLANE):
        pa[t] = jnp.zeros((8, 128), BF)
    spread_a = spread(pa, ra, 1)
    colg_s[0] = pack_column(grad_a, 4, 96)
    colg_s[1] = pack_column(grad_a, 4, 0)
    projected = dot(mix, side_by_side([gated[r] for r in range(4)])).astype(BF).astype(F32)
    projected = jnp.concatenate(
        [projected[:, 128 * r : 128 * (r + 1)][None] for r in range(4)], axis=0
    )
    projected = widen_pairs(projected)
    output = jnp.concatenate(
        [(hidden[:, i] + projected)[:, None] for i in range(2)], axis=1
    ).reshape(16, 32, 128)
    out_ref[...] = jnp.transpose(output.astype(BF), (1, 0, 2))

    def cross(copy, buf, arrived, mine, slots, k):
        copy.wait_recv()
        total = buf[me1].astype(F32)
        for i in range(g1 - 1):
            total = total + arrived[i].astype(F32)
        total = total.astype(BF)
        mine[...] = total
        slots[me2] = total
        for i in range(1, g2):
            send(mine, slots.at[me2], s_send.at[k], s_recv.at[k], line_device(i))
        copy = whole(slots.at[pl.ds(0, g2 - 1)], s_send.at[k], s_recv.at[k])
        departures.append(copy)
        return copy

    def gather(copy, slots, mine, result, k):
        copy.wait_recv()
        total = slots[0].astype(F32)
        for i in range(1, g2):
            total = total + slots[i].astype(F32)
        total = total.astype(BF)
        mine[...] = total
        result[me1] = total
        for i in range(1, g1):
            send(mine, result.at[me1], s_send.at[k], s_recv.at[k], plane_device(i))
        copy = whole(result.at[pl.ds(0, g1 - 1)], s_send.at[k], s_recv.at[k])
        departures.append(copy)
        return copy

    cross_b = cross(spread_b, pb, rb, xb2, rb2, 2)
    cross_a = cross(spread_a, pa, ra, xa2, ra2, 3)
    halo_g = halo_start(
        3, (colg_s.at[0], colg_s.at[1]), (g_s.at[15], g_s.at[0]), rg
    )

    gather_b = gather(cross_b, rb2, xb3, resb, 4)
    gather_a = gather(cross_a, ra2, xa3, resa, 5)

    fine_windows_own(sga, grad_a)
    halo_g.wait_recv()
    fine_windows_rim(sga, rg)
    conv_rows(sga, 16, wa_b, 32, gi_s)
    gi_ref[...] = jnp.transpose(gi_s[...].astype(BF), (1, 0, 2))

    gather_b.wait_recv()
    for ab in range(9):
        for h in range(2):
            rows = slice(16 * h, 16 * h + 16)
            u = 2 * ab + h
            pair = resb[u].astype(F32) * scale
            gkb_ref[3 * ab, rows, :] = pair[:, 0:64]
            gkb_ref[3 * ab + 1, rows, :] = pair[:, 64:128]
            g = u // 9
            rest = resb[18 + u % 9].astype(F32) * scale
            gkb_ref[3 * ab + 2, rows, :] = rest[:, 64 * g : 64 * g + 64]
    last = resb[27].astype(F32) * scale
    gm_ref[0:16, :] = last[:, 0:64]
    gm_ref[16:32, :] = last[:, 64:128]

    gather_a.wait_recv()
    for c in range(3):
        for h in range(4):
            rows = slice(8 * h, 8 * h + 8)
            for l in range(2):
                block = resa[2 * (4 * c + h) + l].astype(F32) * scale
                for q in range(4):
                    gka_ref[(4 * l + q) * 3 + c, rows, :] = block[:, 32 * q : 32 * q + 32]
            rest = resa[24 + h].astype(F32) * scale
            gka_ref[24 + c, rows, :] = rest[:, 32 * c : 32 * c + 32]

    for copy in departures:
        copy.wait_send()


def writer(*refs):
    sems, copies = refs[10], []
    for src, dst in zip(refs[:5], refs[5:10]):
        parts = 3 if src.shape[0] == 27 else 1
        rows = src.shape[0] // parts
        for i in range(parts):
            at = pl.ds(i * rows, rows)
            copies.append(
                pltpu.make_async_copy(src.at[at], dst.at[at], sems.at[len(copies)])
            )
    for copy in copies:
        copy.start()
    for copy in copies:
        copy.wait()


def shards(n_phi, n_eta, features, cotangent, kernel_a, kernel_b, mixing):
    g1, g2 = 4 * n_eta, n_phi // 4
    assert g1 == PLANE
    cells = features.shape[1] * features.shape[2] * n_phi * n_eta
    kernel_b = jnp.swapaxes(kernel_b, 1, 2)
    ins = (features, cotangent, kernel_a, kernel_b, mixing)
    types = (BF, BF, F32, F32, F32)

    def vm(*shape, dtype=BF):
        return pltpu.VMEM(shape, dtype)

    def sums(n):
        return [
            vm(g1, n, 128), vm(g1 - 1, n, 128), vm(n, 128),
            vm(g2, n, 128), vm(n, 128), vm(g1, n, 128),
        ]

    def halo(n):
        return [vm(2 * n + 6, 32, 128)]

    dma = pltpu.SemaphoreType.DMA
    scratch = [
        *[vm(*a.shape) for a in ins], dma((5,)),
        vm(16, 32, 128), vm(2, 4, 32, 128), *halo(4),
        vm(8, 32, 128), vm(2, 2, 32, 128), *halo(2),
        vm(4, 32, 128), vm(2, 32, 128), *halo(4),
        vm(16, 32, 128), vm(2, 4, 32, 128), *halo(4),
        vm(18, 96, 128), vm(16, 128, 288), vm(12, 96, 128), vm(6, 192, 128), vm(18, 96, 128),
        vm(16, 32, 128, dtype=F32), vm(16, 32, 128, dtype=F32), vm(10, 64, 128, dtype=F32),
        vm(4, 32, 128, dtype=F32), vm(16, 32, 128, dtype=F32),
        *sums(8), *sums(16),
        *[dma((k,)) for k in (4, 4, 6, 6)],
    ]
    vmem = pl.BlockSpec(memory_space=pltpu.VMEM)
    anywhere = pl.BlockSpec(memory_space=pl.ANY)
    shapes = [a.shape for a in ins]
    outs = pl.pallas_call(
        functools.partial(kernel, n_phi, n_eta, 1.0 / math.sqrt(cells)),
        out_shape=tuple(pltpu.VMEM(s, t) for s, t in zip(shapes, types)),
        in_specs=[anywhere] * 5,
        out_specs=(vmem,) * 5,
        scratch_shapes=scratch,
        compiler_params=pltpu.CompilerParams(collective_id=0, has_side_effects=True),
        name="block_step",
    )(*ins)
    outs = pl.pallas_call(
        writer,
        out_shape=tuple(jax.ShapeDtypeStruct(s, t) for s, t in zip(shapes, types)),
        in_specs=[vmem] * 5,
        out_specs=(anywhere,) * 5,
        scratch_shapes=[dma((9,))],
        name="write_out",
    )(*[pltpu.with_memory_space_constraint(o, pltpu.VMEM) for o in outs])
    return (*outs[:3], jnp.swapaxes(outs[3], 1, 2), outs[4])


def solution(mesh):
    specs = (P(None, "phi", "eta"), P(None, "phi", "eta"), P(), P(), P())
    body = functools.partial(shards, mesh.shape["phi"], mesh.shape["eta"])
    return jax.shard_map(body, mesh=mesh, in_specs=specs, out_specs=specs, check_vma=False)
```

```python
import functools
import math

import jax
import jax.numpy as jnp
from jax import lax
from jax.experimental import pallas as pl
from jax.experimental.pallas import tpu as pltpu
from jax.sharding import PartitionSpec as P

BF = jnp.bfloat16
F32 = jnp.float32
MESH = pl.DeviceIdType.MESH
DIRS = ((0, 1), (0, -1), (1, 0), (1, 1), (1, -1), (-1, 0), (-1, 1), (-1, -1))
PLANE = 32


def lane_of(shape):
    return lax.broadcasted_iota(jnp.int32, shape, len(shape) - 1)


def roll(x, shift):
    shift %= 128
    return x if shift == 0 else pltpu.roll(x, shift, x.ndim - 1)


def dot(a, b):
    return jnp.dot(a, b, preferred_element_type=F32)


def dot_nt(a, b):
    return lax.dot_general(a, b, (((1,), (1,)), ((), ())), preferred_element_type=F32)


def zero(x):
    return jnp.zeros((), x.dtype)


def side_by_side(rows):
    return jnp.concatenate(rows, axis=1)


def by_quarter(v0, v1, v2, v3):
    lane = lane_of(v0.shape)
    return jnp.where(
        lane < 64, jnp.where(lane < 32, v0, v1), jnp.where(lane < 96, v2, v3)
    )


def pack_column(x, size, start):
    return by_quarter(
        *[roll(x[size * g : size * (g + 1)], 32 * g - start) for g in range(4)]
    )


def unpack_column(packed, want):
    return [roll(packed, want - 32 * g) for g in range(4)]


def pack_pair(x, y):
    return jnp.where(lane_of(x.shape) < 64, roll(x, -32), roll(y, 32))


def widen_pairs(x):
    up, down, across = roll(x, 32), roll(x, -32), roll(x, 64)
    low, high = by_quarter(x, up, up, across), by_quarter(across, down, down, x)
    return jnp.concatenate([low, high], axis=0)


def pool_columns(x):
    lane = lane_of(x.shape)
    both = x + jnp.where(lane < 64, roll(x, 32), roll(x, -32))
    return jnp.where((lane >= 32) & (lane < 96), both, zero(x))


def layer_shifts(x):
    layer = lane_of(x.shape) % 32
    return [
        jnp.where(layer < 31, roll(x, -1), zero(x)),
        x,
        jnp.where(layer > 0, roll(x, 1), zero(x)),
    ]


def conv_rows(src, count, weight, outs, sink):
    layer = lane_of((outs, 128)) % 32
    flat = 3 * src.shape[1]
    for r in range(0, count, 2):
        pair = [src[r + i : r + i + 3].reshape(flat, 128) for i in range(2)]
        z = dot(weight, side_by_side(pair))
        for i in range(2):
            zi = z[:, 128 * i : 128 * (i + 1)]
            low = jnp.where(layer > 0, roll(zi[:outs], 1), 0.0)
            high = jnp.where(layer < 31, roll(zi[2 * outs :], -1), 0.0)
            sink[r + i] = zi[outs : 2 * outs] + low + high


def sigmoid(v):
    return 1.0 / (1.0 + jnp.exp(-v))


def kernel(n_phi, n_eta, scale, *refs):
    ins, (out_ref, gi_ref, gka_ref, gkb_ref, gm_ref) = refs[:5], refs[5:10]
    (
        f_ref, ct_ref, ka_ref, kb_ref, mix_ref, load_sem,
        x_s, colx_s, rx,
        fold_s, colf_s, rf,
        colc_s, rowc_s, rc,
        g_s, colg_s, rg,
        sfa, sft, scb, sgb, sga, slope_a_s, lin_a_s, lin_b_s, gc_s, gi_s,
        pa, ra, xa2, ra2, xa3, resa, pb, rb, xb2, rb2, xb3, resb,
        h_send, h_recv, s_send, s_recv,
    ) = refs[10:]
    p = lax.axis_index("phi")
    e = lax.axis_index("eta")
    g1, g2 = 4 * n_eta, n_phi // 4
    me2 = p // 4

    def wrap(i, n):
        return jnp.where(i >= n, i - n, i)

    in_plane = lax.rem(p, 4)
    plane_p = [wrap(in_plane + i, 4) for i in range(4)]
    phi_of = [me2 * 4 + i for i in plane_p]
    eta_of = [wrap(e + i, n_eta) for i in range(n_eta)]
    line_of = [wrap(p + 4 * i, n_phi) for i in range(g2)]
    near_of = {0: p, 1: wrap(p + 1, n_phi), -1: wrap(p + n_phi - 1, n_phi)}
    me1 = in_plane * n_eta + e
    steps = [(i, j) for i in range(4) for j in range(n_eta) if i or j]
    steps.sort(key=lambda ij: (-min(ij[1], n_eta - ij[1]), -min(ij[0], 4 - ij[0])))

    def halo_device(d):
        return (near_of[d[0]], eta_of[d[1] % n_eta])

    def plane_device(step):
        return (phi_of[step[0]], eta_of[step[1]])

    def line_device(i):
        return (line_of[i], e)

    loads = [
        pltpu.make_async_copy(src, dst, load_sem.at[k])
        for k, (src, dst) in enumerate(zip(ins, (f_ref, ct_ref, ka_ref, kb_ref, mix_ref)))
    ]
    loads[0].start()

    barrier = pltpu.get_barrier_semaphore()
    targets = [line_device(i) for i in sorted(range(1, g2), key=lambda i: -min(i, g2 - i))]
    planes = [plane_device(step) for step in steps]
    targets += planes[:12] + [halo_device(d) for d in DIRS] + planes[12:]
    for target in targets:
        pl.semaphore_signal(barrier, inc=1, device_id=target, device_id_type=MESH)
    for load in loads[1:]:
        load.start()

    departures = []

    def send(src, dst, ssem, rsem, target):
        pltpu.make_async_remote_copy(
            src_ref=src, dst_ref=dst, send_sem=ssem, recv_sem=rsem,
            device_id=target, device_id_type=MESH,
        ).start()

    def whole(ref, ssem, rsem):
        return pltpu.make_async_remote_copy(
            src_ref=ref, dst_ref=ref, send_sem=ssem, recv_sem=rsem,
            device_id=(p, e), device_id_type=MESH,
        )

    def halo_start(which, cols, rows, arrived):
        n = (arrived.shape[0] - 6) // 2
        ssem, rsem = h_send.at[which], h_recv.at[which]
        for k, d in sorted(enumerate(DIRS), key=lambda kd: -abs(kd[1][0]) - abs(kd[1][1])):
            if k < 2:
                src, dst = cols[k], arrived.at[pl.ds(n * k, n)]
            else:
                src, dst = rows[0 if d[0] > 0 else 1], arrived.at[2 * n + k - 2]
            send(src, dst, ssem, rsem, halo_device(d))
        copy = whole(arrived, ssem, rsem)
        departures.append(copy)
        return copy

    def halo_parts(arrived):
        n = (arrived.shape[0] - 6) // 2
        rows = [arrived[2 * n + j : 2 * n + j + 1] for j in range(6)]
        return (arrived[0:n], arrived[n : 2 * n]), rows

    has_left = e > 0
    has_right = e < n_eta - 1
    lo32 = jnp.where(has_left, 32, 0)
    lo64 = jnp.where(has_left, 64, 0)
    hi96 = jnp.where(has_right, 96, 128)
    hi64 = jnp.where(has_right, 64, 128)

    loads[0].wait()
    x = jnp.transpose(f_ref[...], (1, 0, 2))
    x_s[...] = x
    colx_s[0] = pack_column(x, 4, 96)
    colx_s[1] = pack_column(x, 4, 0)
    pl.semaphore_wait(barrier, len(targets))
    halo_x = halo_start(
        0, (colx_s.at[0], colx_s.at[1]), (x_s.at[15], x_s.at[0]), rx
    )

    for load in loads[1:]:
        load.wait()
    ct = jnp.transpose(ct_ref[...], (1, 0, 2)).astype(F32).reshape(8, 2, 32, 128)
    fold = pool_columns(ct[:, 0] + ct[:, 1]).astype(BF)
    fold_s[...] = fold
    colf_s[0] = pack_column(fold, 2, 64)
    colf_s[1] = pack_column(fold, 2, 32)
    halo_f = halo_start(
        1, (colf_s.at[0], colf_s.at[1]), (fold_s.at[7], fold_s.at[0]), rf
    )

    def forward_weight(ref):
        return jnp.concatenate(
            [side_by_side([ref[3 * ab + c] for ab in range(9)]) for c in range(3)], axis=0
        )

    def backward_weight(ref):
        return jnp.concatenate(
            [side_by_side([ref[26 - 3 * ab - c] for c in range(3)]) for ab in range(9)], axis=0
        ).T

    wa_f, wa_b = forward_weight(ka_ref), backward_weight(ka_ref)
    wb_f = jnp.concatenate(
        [side_by_side([kb_ref[3 * ab + c] for c in range(3)]) for ab in range(9)], axis=0
    ).T
    wb_b = jnp.concatenate(
        [side_by_side([kb_ref[26 - 3 * ab - c] for ab in range(9)]) for c in range(3)], axis=0
    )
    mix = mix_ref[...]
    mix_t = mix.T

    def fine_windows_own(dst, rows):
        lane = lane_of(rows.shape)
        dst[1:17, 0:32, :] = jnp.where(lane < 32, zero(rows), roll(rows, 32))
        dst[1:17, 32:64, :] = rows
        dst[1:17, 64:96, :] = jnp.where(lane >= 96, zero(rows), roll(rows, -32))

    def fine_windows_rim(dst, arrived):
        cols, rim = halo_parts(arrived)
        lane = lane_of((16, 32, 128))
        left = jnp.concatenate(unpack_column(cols[0], 0), axis=0)
        right = jnp.concatenate(unpack_column(cols[1], 96), axis=0)
        dst[1:17, 0:32, :] = jnp.where(lane < lo32, left, dst[1:17, 0:32, :])
        dst[1:17, 64:96, :] = jnp.where(lane >= hi96, right, dst[1:17, 64:96, :])
        lane = lane_of((1, 32, 128))
        for k, at in ((0, 0), (3, 17)):
            rows, left, right = rim[k], roll(rim[k + 1], 32), roll(rim[k + 2], 96)
            dst[at : at + 1, 0:32, :] = jnp.where(
                lane < lo32, left, jnp.where(lane < 32, zero(rows), roll(rows, 32))
            )
            dst[at : at + 1, 32:64, :] = rows
            dst[at : at + 1, 64:96, :] = jnp.where(
                lane >= hi96, right, jnp.where(lane >= 96, zero(rows), roll(rows, -32))
            )

    fine_windows_own(sfa, x)

    halo_x.wait_recv()
    fine_windows_rim(sfa, rx)
    conv_rows(sfa, 16, wa_f, 32, lin_a_s)
    lin_a = lin_a_s[...]
    hidden = (lin_a / (1.0 + jnp.exp(-lin_a))).astype(BF).astype(F32).reshape(8, 2, 32, 128)
    coarse = (0.25 * pool_columns(hidden[:, 0] + hidden[:, 1])).astype(BF)

    colc_s[...] = pack_pair(coarse[0:4], coarse[4:8])
    rowc_s[0:1] = pack_pair(coarse[6:7], coarse[7:8])
    rowc_s[1:2] = pack_pair(coarse[0:1], coarse[1:2])
    halo_c = halo_start(2, (colc_s, colc_s), (rowc_s.at[0], rowc_s.at[1]), rc)

    halo_f.wait_recv()
    cols, rim = halo_parts(rf)
    fold_rows = jnp.concatenate([rim[0], fold, rim[3]], axis=0)
    fold_left = jnp.concatenate(
        [roll(rim[1], 64)] + unpack_column(cols[0], 0) + [roll(rim[4], 64)], axis=0
    )
    fold_right = jnp.concatenate(
        [roll(rim[2], 64)] + unpack_column(cols[1], 96) + [roll(rim[5], 64)], axis=0
    )
    lane = lane_of(fold_rows.shape)
    fold_wide = jnp.where(
        (lane >= 32) & (lane < 96),
        fold_rows,
        jnp.where(
            lane < lo32, fold_left, jnp.where(lane >= hi96, fold_right, zero(fold_rows))
        ),
    )

    fold_pairs = pack_pair(fold[0:4], fold[4:8])
    grad_gated = dot(mix_t, side_by_side([fold_wide[r] for r in range(10)]))
    sig_a = sigmoid(lin_a)
    slope_a_s[...] = sig_a * (1.0 + lin_a * (1.0 - sig_a))

    own_rows = slice(2, 10)
    lane = lane_of(coarse.shape)
    scb[own_rows, 0:32, :] = jnp.where(lane < 64, zero(coarse), roll(coarse, 32))
    scb[own_rows, 32:64, :] = coarse
    scb[own_rows, 64:96, :] = jnp.where(lane < 64, roll(coarse, -32), zero(coarse))

    for r in range(16):
        sft[r] = sfa[r : r + 3].reshape(288, 128).T

    halo_c.wait_recv()
    cols, rim = halo_parts(rc)

    def two(*parts):
        return jnp.concatenate(parts, axis=0)

    left, right = two(cols[0], roll(cols[0], 64)), two(roll(cols[1], 64), cols[1])
    left = jnp.where(lane < lo64, left, zero(left))
    right = jnp.where(lane >= hi64, right, zero(right))
    scb[own_rows, 0:32, :] = jnp.where(lane < 64, left, scb[own_rows, 0:32, :])
    scb[own_rows, 32:64, :] = jnp.where(
        lane < 32, roll(left, -32), jnp.where(lane < 96, coarse, roll(right, 32))
    )
    scb[own_rows, 64:96, :] = jnp.where(lane < 64, scb[own_rows, 64:96, :], right)
    lane = lane_of((2, 32, 128))
    for k, at in ((0, 0), (3, 10)):
        rows = two(roll(rim[k], 32), roll(rim[k], -32))
        left, right = two(rim[k + 1], roll(rim[k + 1], 64)), two(roll(rim[k + 2], 64), rim[k + 2])
        left = jnp.where(lane < lo64, left, zero(left))
        right = jnp.where(lane >= hi64, right, zero(right))
        scb[at : at + 2, 0:32, :] = jnp.where(lane < 64, left, roll(rows, 32))
        scb[at : at + 2, 32:64, :] = jnp.where(
            lane < 32, roll(left, -32), jnp.where(lane < 96, rows, roll(right, 32))
        )
        scb[at : at + 2, 64:96, :] = jnp.where(lane < 64, roll(rows, -32), right)

    conv_rows(scb, 10, wb_f, 64, lin_b_s)
    lin_b = lin_b_s[...]
    sig_b = sigmoid(lin_b)
    slope_b = sig_b * (1.0 + lin_b * (1.0 - sig_b))
    gated = (lin_b * sig_b)[1:9].astype(BF)
    grad_b = jnp.concatenate(
        [(grad_gated[:, 128 * r : 128 * (r + 1)] * slope_b[r]).astype(BF)[None] for r in range(10)],
        axis=0,
    )
    top, low = grad_b[0:6], grad_b[4:10]
    lane = lane_of(top.shape)
    sgb[:, 0:64, :] = jnp.where(lane < 64, top, roll(low, 64))
    sgb[:, 64:128, :] = pack_pair(top, low)
    sgb[:, 128:192, :] = jnp.where(lane < 64, roll(top, 64), low)

    shifts = layer_shifts(sgb[1:5, 64:128, :])
    up = side_by_side([jnp.concatenate([s[r] for s in shifts], axis=0) for r in range(4)])
    seen = pack_pair(scb[1:7], scb[5:11])
    seen = side_by_side([seen[r : r + 3].reshape(288, 128) for r in range(4)])
    gated = pack_pair(gated[0:4], gated[4:8])
    sum_b = dot_nt(seen, up)
    sum_m = dot_nt(
        side_by_side([fold_pairs[r] for r in range(4)]), side_by_side([gated[r] for r in range(4)])
    )
    for i in range(18):
        pb[i] = sum_b[16 * i : 16 * i + 16, 0:128].astype(BF)
    rest = side_by_side([sum_b[144 * g : 144 * g + 144, 128:192] for g in range(2)])
    for i in range(9):
        pb[18 + i] = rest[16 * i : 16 * i + 16].astype(BF)
    pb[27] = side_by_side([sum_m[0:16], sum_m[16:32]]).astype(BF)
    for t in range(28, PLANE):
        pb[t] = jnp.zeros((16, 128), BF)

    def spread(buf, dst, k):
        for i, step in enumerate(steps):
            q = plane_p[step[0]] * n_eta + eta_of[step[1]]
            send(buf.at[q], dst.at[i], s_send.at[k], s_recv.at[k], plane_device(step))
        copy = whole(dst, s_send.at[k], s_recv.at[k])
        departures.append(copy)
        return copy

    spread_b = spread(pb, rb, 0)

    conv_rows(sgb, 4, wb_b, 32, gc_s)
    grad_coarse = widen_pairs(gc_s[...].astype(BF).astype(F32))
    grad_hidden = jnp.concatenate(
        [(ct[:, i] + 0.25 * grad_coarse)[:, None] for i in range(2)], axis=1
    ).reshape(16, 32, 128)
    grad_a = (grad_hidden * slope_a_s[...]).astype(BF)
    g_s[...] = grad_a
    shifts = layer_shifts(grad_a)
    up = side_by_side([jnp.concatenate([s[r] for s in shifts], axis=0) for r in range(16)])
    sum_a = dot(up, sft[...].reshape(2048, 288))
    for i in range(12):
        for l in range(2):
            pa[2 * i + l] = sum_a[8 * i : 8 * i + 8, 128 * l : 128 * l + 128].astype(BF)
    rest = side_by_side([sum_a[32 * g : 32 * g + 32, 256:288] for g in range(3)])
    rest = jnp.concatenate([rest, jnp.zeros((32, 32), F32)], axis=1)
    for i in range(4):
        pa[24 + i] = rest[8 * i : 8 * i + 8].astype(BF)
    for t in range(28, PLANE):
        pa[t] = jnp.zeros((8, 128), BF)
    spread_a = spread(pa, ra, 1)
    colg_s[0] = pack_column(grad_a, 4, 96)
    colg_s[1] = pack_column(grad_a, 4, 0)
    projected = dot(mix, side_by_side([gated[r] for r in range(4)])).astype(BF).astype(F32)
    projected = jnp.concatenate(
        [projected[:, 128 * r : 128 * (r + 1)][None] for r in range(4)], axis=0
    )
    projected = widen_pairs(projected)
    output = jnp.concatenate(
        [(hidden[:, i] + projected)[:, None] for i in range(2)], axis=1
    ).reshape(16, 32, 128)
    out_ref[...] = jnp.transpose(output.astype(BF), (1, 0, 2))

    def cross(copy, buf, arrived, mine, slots, k):
        copy.wait_recv()
        total = buf[me1].astype(F32)
        for i in range(g1 - 1):
            total = total + arrived[i].astype(F32)
        total = total.astype(BF)
        mine[...] = total
        slots[me2] = total
        for i in range(1, g2):
            send(mine, slots.at[me2], s_send.at[k], s_recv.at[k], line_device(i))
        copy = whole(slots.at[pl.ds(0, g2 - 1)], s_send.at[k], s_recv.at[k])
        departures.append(copy)
        return copy

    def gather(copy, slots, mine, result, k):
        copy.wait_recv()
        total = slots[0].astype(F32)
        for i in range(1, g2):
            total = total + slots[i].astype(F32)
        total = total.astype(BF)
        mine[...] = total
        result[me1] = total
        for step in steps:
            send(mine, result.at[me1], s_send.at[k], s_recv.at[k], plane_device(step))
        copy = whole(result.at[pl.ds(0, g1 - 1)], s_send.at[k], s_recv.at[k])
        departures.append(copy)
        return copy

    cross_b = cross(spread_b, pb, rb, xb2, rb2, 2)
    cross_a = cross(spread_a, pa, ra, xa2, ra2, 3)
    halo_g = halo_start(
        3, (colg_s.at[0], colg_s.at[1]), (g_s.at[15], g_s.at[0]), rg
    )

    gather_b = gather(cross_b, rb2, xb3, resb, 4)
    gather_a = gather(cross_a, ra2, xa3, resa, 5)

    fine_windows_own(sga, grad_a)
    halo_g.wait_recv()
    fine_windows_rim(sga, rg)
    conv_rows(sga, 16, wa_b, 32, gi_s)
    gi_ref[...] = jnp.transpose(gi_s[...].astype(BF), (1, 0, 2))

    gather_b.wait_recv()
    for ab in range(9):
        for h in range(2):
            rows = slice(16 * h, 16 * h + 16)
            u = 2 * ab + h
            pair = resb[u].astype(F32) * scale
            gkb_ref[3 * ab, rows, :] = pair[:, 0:64]
            gkb_ref[3 * ab + 1, rows, :] = pair[:, 64:128]
            g = u // 9
            rest = resb[18 + u % 9].astype(F32) * scale
            gkb_ref[3 * ab + 2, rows, :] = rest[:, 64 * g : 64 * g + 64]
    last = resb[27].astype(F32) * scale
    gm_ref[0:16, :] = last[:, 0:64]
    gm_ref[16:32, :] = last[:, 64:128]

    gather_a.wait_recv()
    for c in range(3):
        for h in range(4):
            rows = slice(8 * h, 8 * h + 8)
            for l in range(2):
                block = resa[2 * (4 * c + h) + l].astype(F32) * scale
                for q in range(4):
                    gka_ref[(4 * l + q) * 3 + c, rows, :] = block[:, 32 * q : 32 * q + 32]
            rest = resa[24 + h].astype(F32) * scale
            gka_ref[24 + c, rows, :] = rest[:, 32 * c : 32 * c + 32]

    for copy in departures:
        copy.wait_send()


def writer(*refs):
    sems, copies = refs[10], []
    for src, dst in zip(refs[:5], refs[5:10]):
        parts = 3 if src.shape[0] == 27 else 1
        rows = src.shape[0] // parts
        for i in range(parts):
            at = pl.ds(i * rows, rows)
            copies.append(
                pltpu.make_async_copy(src.at[at], dst.at[at], sems.at[len(copies)])
            )
    for copy in copies:
        copy.start()
    for copy in copies:
        copy.wait()


def shards(n_phi, n_eta, features, cotangent, kernel_a, kernel_b, mixing):
    g1, g2 = 4 * n_eta, n_phi // 4
    assert g1 == PLANE
    cells = features.shape[1] * features.shape[2] * n_phi * n_eta
    kernel_b = jnp.swapaxes(kernel_b, 1, 2)
    ins = (features, cotangent, kernel_a, kernel_b, mixing)
    types = (BF, BF, F32, F32, F32)

    def vm(*shape, dtype=BF):
        return pltpu.VMEM(shape, dtype)

    def sums(n):
        return [
            vm(g1, n, 128), vm(g1 - 1, n, 128), vm(n, 128),
            vm(g2, n, 128), vm(n, 128), vm(g1, n, 128),
        ]

    def halo(n):
        return [vm(2 * n + 6, 32, 128)]

    dma = pltpu.SemaphoreType.DMA
    scratch = [
        *[vm(*a.shape) for a in ins], dma((5,)),
        vm(16, 32, 128), vm(2, 4, 32, 128), *halo(4),
        vm(8, 32, 128), vm(2, 2, 32, 128), *halo(2),
        vm(4, 32, 128), vm(2, 32, 128), *halo(4),
        vm(16, 32, 128), vm(2, 4, 32, 128), *halo(4),
        vm(18, 96, 128), vm(16, 128, 288), vm(12, 96, 128), vm(6, 192, 128), vm(18, 96, 128),
        vm(16, 32, 128, dtype=F32), vm(16, 32, 128, dtype=F32), vm(10, 64, 128, dtype=F32),
        vm(4, 32, 128, dtype=F32), vm(16, 32, 128, dtype=F32),
        *sums(8), *sums(16),
        *[dma((k,)) for k in (4, 4, 6, 6)],
    ]
    vmem = pl.BlockSpec(memory_space=pltpu.VMEM)
    anywhere = pl.BlockSpec(memory_space=pl.ANY)
    shapes = [a.shape for a in ins]
    outs = pl.pallas_call(
        functools.partial(kernel, n_phi, n_eta, 1.0 / math.sqrt(cells)),
        out_shape=tuple(pltpu.VMEM(s, t) for s, t in zip(shapes, types)),
        in_specs=[anywhere] * 5,
        out_specs=(vmem,) * 5,
        scratch_shapes=scratch,
        compiler_params=pltpu.CompilerParams(collective_id=0, has_side_effects=True),
        name="block_step",
    )(*ins)
    outs = pl.pallas_call(
        writer,
        out_shape=tuple(jax.ShapeDtypeStruct(s, t) for s, t in zip(shapes, types)),
        in_specs=[vmem] * 5,
        out_specs=(anywhere,) * 5,
        scratch_shapes=[dma((9,))],
        name="write_out",
    )(*[pltpu.with_memory_space_constraint(o, pltpu.VMEM) for o in outs])
    return (*outs[:3], jnp.swapaxes(outs[3], 1, 2), outs[4])


def solution(mesh):
    specs = (P(None, "phi", "eta"), P(None, "phi", "eta"), P(), P(), P())
    body = functools.partial(shards, mesh.shape["phi"], mesh.shape["eta"])
    return jax.shard_map(body, mesh=mesh, in_specs=specs, out_specs=specs, check_vma=False)
```

```python
import functools
import math

import jax
import jax.numpy as jnp
from jax import lax
from jax.experimental import pallas as pl
from jax.experimental.pallas import tpu as pltpu
from jax.sharding import PartitionSpec as P

BF = jnp.bfloat16
F32 = jnp.float32
MESH = pl.DeviceIdType.MESH
DIRS = ((0, 1), (0, -1), (1, 0), (1, 1), (1, -1), (-1, 0), (-1, 1), (-1, -1))
PLANE = 32


def lane_of(shape):
    return lax.broadcasted_iota(jnp.int32, shape, len(shape) - 1)


def roll(x, shift):
    shift %= 128
    return x if shift == 0 else pltpu.roll(x, shift, x.ndim - 1)


def dot(a, b):
    return jnp.dot(a, b, preferred_element_type=F32)


def dot_nt(a, b):
    return lax.dot_general(a, b, (((1,), (1,)), ((), ())), preferred_element_type=F32)


def zero(x):
    return jnp.zeros((), x.dtype)


def side_by_side(rows):
    return jnp.concatenate(rows, axis=1)


def by_quarter(v0, v1, v2, v3):
    lane = lane_of(v0.shape)
    return jnp.where(
        lane < 64, jnp.where(lane < 32, v0, v1), jnp.where(lane < 96, v2, v3)
    )


def pack_column(x, size, start):
    return by_quarter(
        *[roll(x[size * g : size * (g + 1)], 32 * g - start) for g in range(4)]
    )


def unpack_column(packed, want):
    return [roll(packed, want - 32 * g) for g in range(4)]


def pack_pair(x, y):
    return jnp.where(lane_of(x.shape) < 64, roll(x, -32), roll(y, 32))


def widen_pairs(x):
    up, down, across = roll(x, 32), roll(x, -32), roll(x, 64)
    low, high = by_quarter(x, up, up, across), by_quarter(across, down, down, x)
    return jnp.concatenate([low, high], axis=0)


def pool_columns(x):
    lane = lane_of(x.shape)
    both = x + jnp.where(lane < 64, roll(x, 32), roll(x, -32))
    return jnp.where((lane >= 32) & (lane < 96), both, zero(x))


def layer_shifts(x):
    layer = lane_of(x.shape) % 32
    return [
        jnp.where(layer < 31, roll(x, -1), zero(x)),
        x,
        jnp.where(layer > 0, roll(x, 1), zero(x)),
    ]


def conv_rows(src, count, weight, outs, sink):
    layer = lane_of((outs, 128)) % 32
    flat = 3 * src.shape[1]
    for r in range(0, count, 2):
        pair = [src[r + i : r + i + 3].reshape(flat, 128) for i in range(2)]
        z = dot(weight, side_by_side(pair))
        for i in range(2):
            zi = z[:, 128 * i : 128 * (i + 1)]
            low = jnp.where(layer > 0, roll(zi[:outs], 1), 0.0)
            high = jnp.where(layer < 31, roll(zi[2 * outs :], -1), 0.0)
            sink[r + i] = zi[outs : 2 * outs] + low + high


def sigmoid(v):
    return 1.0 / (1.0 + jnp.exp(-v))


def kernel(n_phi, n_eta, scale, *refs):
    ins, (out_ref, gi_ref, gka_ref, gkb_ref, gm_ref) = refs[:5], refs[5:10]
    (
        f_ref, ct_ref, ka_ref, kb_ref, mix_ref, load_sem,
        x_s, colx_s, rx,
        fold_s, colf_s, rf,
        colc_s, rowc_s, rc,
        g_s, colg_s, rg,
        sfa, sft, scb, sgb, sga, slope_a_s, lin_a_s, lin_b_s, gc_s, gi_s,
        pa, ra, xa2, ra2, xa3, resa, pb, rb, xb2, rb2, xb3, resb,
        h_send, h_recv, s_send, s_recv,
    ) = refs[10:]
    p = lax.axis_index("phi")
    e = lax.axis_index("eta")
    g1, g2 = 4 * n_eta, n_phi // 4
    me2 = p // 4

    def wrap(i, n):
        return jnp.where(i >= n, i - n, i)

    in_plane = lax.rem(p, 4)
    plane_p = [wrap(in_plane + i, 4) for i in range(4)]
    phi_of = [me2 * 4 + i for i in plane_p]
    eta_of = [wrap(e + i, n_eta) for i in range(n_eta)]
    line_of = [wrap(p + 4 * i, n_phi) for i in range(g2)]
    near_of = {0: p, 1: wrap(p + 1, n_phi), -1: wrap(p + n_phi - 1, n_phi)}
    me1 = in_plane * n_eta + e
    steps = [(i, j) for i in range(4) for j in range(n_eta) if i or j]
    steps.sort(key=lambda ij: (-min(ij[1], n_eta - ij[1]), -min(ij[0], 4 - ij[0])))

    def halo_device(d):
        return (near_of[d[0]], eta_of[d[1] % n_eta])

    def plane_device(step):
        return (phi_of[step[0]], eta_of[step[1]])

    def line_device(i):
        return (line_of[i], e)

    loads = [
        pltpu.make_async_copy(src, dst, load_sem.at[k])
        for k, (src, dst) in enumerate(zip(ins, (f_ref, ct_ref, ka_ref, kb_ref, mix_ref)))
    ]
    loads[0].start()

    barrier = pltpu.get_barrier_semaphore()
    targets = [line_device(i) for i in sorted(range(1, g2), key=lambda i: -min(i, g2 - i))]
    planes = [plane_device(step) for step in steps]
    targets += planes[:12] + [halo_device(d) for d in DIRS] + planes[12:]
    for target in targets:
        pl.semaphore_signal(barrier, inc=1, device_id=target, device_id_type=MESH)
    for load in loads[1:]:
        load.start()

    departures = []

    def send(src, dst, ssem, rsem, target):
        pltpu.make_async_remote_copy(
            src_ref=src, dst_ref=dst, send_sem=ssem, recv_sem=rsem,
            device_id=target, device_id_type=MESH,
        ).start()

    def whole(ref, ssem, rsem):
        return pltpu.make_async_remote_copy(
            src_ref=ref, dst_ref=ref, send_sem=ssem, recv_sem=rsem,
            device_id=(p, e), device_id_type=MESH,
        )

    def halo_start(which, cols, rows, arrived):
        n = (arrived.shape[0] - 6) // 2
        ssem, rsem = h_send.at[which], h_recv.at[which]
        for k, d in sorted(enumerate(DIRS), key=lambda kd: -abs(kd[1][0]) - abs(kd[1][1])):
            if k < 2:
                src, dst = cols[k], arrived.at[pl.ds(n * k, n)]
            else:
                src, dst = rows[0 if d[0] > 0 else 1], arrived.at[2 * n + k - 2]
            send(src, dst, ssem, rsem, halo_device(d))
        copy = whole(arrived, ssem, rsem)
        departures.append(copy)
        return copy

    def halo_parts(arrived):
        n = (arrived.shape[0] - 6) // 2
        rows = [arrived[2 * n + j : 2 * n + j + 1] for j in range(6)]
        return (arrived[0:n], arrived[n : 2 * n]), rows

    has_left = e > 0
    has_right = e < n_eta - 1
    lo32 = jnp.where(has_left, 32, 0)
    lo64 = jnp.where(has_left, 64, 0)
    hi96 = jnp.where(has_right, 96, 128)
    hi64 = jnp.where(has_right, 64, 128)

    loads[0].wait()
    x = jnp.transpose(f_ref[...], (1, 0, 2))
    x_s[...] = x
    colx_s[0] = pack_column(x, 4, 96)
    colx_s[1] = pack_column(x, 4, 0)
    pl.semaphore_wait(barrier, len(targets))
    halo_x = halo_start(
        0, (colx_s.at[0], colx_s.at[1]), (x_s.at[15], x_s.at[0]), rx
    )

    for load in loads[1:]:
        load.wait()
    ct = jnp.transpose(ct_ref[...], (1, 0, 2)).astype(F32).reshape(8, 2, 32, 128)
    fold = pool_columns(ct[:, 0] + ct[:, 1]).astype(BF)
    fold_s[...] = fold
    colf_s[0] = pack_column(fold, 2, 64)
    colf_s[1] = pack_column(fold, 2, 32)

    def forward_weight(ref):
        return jnp.concatenate(
            [side_by_side([ref[3 * ab + c] for ab in range(9)]) for c in range(3)], axis=0
        )

    def backward_weight(ref):
        return jnp.concatenate(
            [side_by_side([ref[26 - 3 * ab - c] for c in range(3)]) for ab in range(9)], axis=0
        ).T

    wa_f, wa_b = forward_weight(ka_ref), backward_weight(ka_ref)
    wb_f = jnp.concatenate(
        [side_by_side([kb_ref[3 * ab + c] for c in range(3)]) for ab in range(9)], axis=0
    ).T
    wb_b = jnp.concatenate(
        [side_by_side([kb_ref[26 - 3 * ab - c] for ab in range(9)]) for c in range(3)], axis=0
    )
    mix = mix_ref[...]
    mix_t = mix.T

    def fine_windows_own(dst, rows):
        lane = lane_of(rows.shape)
        dst[1:17, 0:32, :] = jnp.where(lane < 32, zero(rows), roll(rows, 32))
        dst[1:17, 32:64, :] = rows
        dst[1:17, 64:96, :] = jnp.where(lane >= 96, zero(rows), roll(rows, -32))

    def fine_windows_rim(dst, arrived):
        cols, rim = halo_parts(arrived)
        lane = lane_of((16, 32, 128))
        left = jnp.concatenate(unpack_column(cols[0], 0), axis=0)
        right = jnp.concatenate(unpack_column(cols[1], 96), axis=0)
        dst[1:17, 0:32, :] = jnp.where(lane < lo32, left, dst[1:17, 0:32, :])
        dst[1:17, 64:96, :] = jnp.where(lane >= hi96, right, dst[1:17, 64:96, :])
        lane = lane_of((1, 32, 128))
        for k, at in ((0, 0), (3, 17)):
            rows, left, right = rim[k], roll(rim[k + 1], 32), roll(rim[k + 2], 96)
            dst[at : at + 1, 0:32, :] = jnp.where(
                lane < lo32, left, jnp.where(lane < 32, zero(rows), roll(rows, 32))
            )
            dst[at : at + 1, 32:64, :] = rows
            dst[at : at + 1, 64:96, :] = jnp.where(
                lane >= hi96, right, jnp.where(lane >= 96, zero(rows), roll(rows, -32))
            )

    fine_windows_own(sfa, x)

    halo_x.wait_send()
    departures.remove(halo_x)
    halo_f = halo_start(
        1, (colf_s.at[0], colf_s.at[1]), (fold_s.at[7], fold_s.at[0]), rf
    )
    halo_x.wait_recv()
    fine_windows_rim(sfa, rx)
    conv_rows(sfa, 16, wa_f, 32, lin_a_s)
    lin_a = lin_a_s[...]
    hidden = (lin_a / (1.0 + jnp.exp(-lin_a))).astype(BF).astype(F32).reshape(8, 2, 32, 128)
    coarse = (0.25 * pool_columns(hidden[:, 0] + hidden[:, 1])).astype(BF)

    colc_s[...] = pack_pair(coarse[0:4], coarse[4:8])
    rowc_s[0:1] = pack_pair(coarse[6:7], coarse[7:8])
    rowc_s[1:2] = pack_pair(coarse[0:1], coarse[1:2])
    halo_c = halo_start(2, (colc_s, colc_s), (rowc_s.at[0], rowc_s.at[1]), rc)

    halo_f.wait_recv()
    cols, rim = halo_parts(rf)
    fold_rows = jnp.concatenate([rim[0], fold, rim[3]], axis=0)
    fold_left = jnp.concatenate(
        [roll(rim[1], 64)] + unpack_column(cols[0], 0) + [roll(rim[4], 64)], axis=0
    )
    fold_right = jnp.concatenate(
        [roll(rim[2], 64)] + unpack_column(cols[1], 96) + [roll(rim[5], 64)], axis=0
    )
    lane = lane_of(fold_rows.shape)
    fold_wide = jnp.where(
        (lane >= 32) & (lane < 96),
        fold_rows,
        jnp.where(
            lane < lo32, fold_left, jnp.where(lane >= hi96, fold_right, zero(fold_rows))
        ),
    )

    fold_pairs = pack_pair(fold[0:4], fold[4:8])
    grad_gated = dot(mix_t, side_by_side([fold_wide[r] for r in range(10)]))
    sig_a = sigmoid(lin_a)
    slope_a_s[...] = sig_a * (1.0 + lin_a * (1.0 - sig_a))

    own_rows = slice(2, 10)
    lane = lane_of(coarse.shape)
    scb[own_rows, 0:32, :] = jnp.where(lane < 64, zero(coarse), roll(coarse, 32))
    scb[own_rows, 32:64, :] = coarse
    scb[own_rows, 64:96, :] = jnp.where(lane < 64, roll(coarse, -32), zero(coarse))

    for r in range(16):
        sft[r] = sfa[r : r + 3].reshape(288, 128).T

    halo_c.wait_recv()
    cols, rim = halo_parts(rc)

    def two(*parts):
        return jnp.concatenate(parts, axis=0)

    left, right = two(cols[0], roll(cols[0], 64)), two(roll(cols[1], 64), cols[1])
    left = jnp.where(lane < lo64, left, zero(left))
    right = jnp.where(lane >= hi64, right, zero(right))
    scb[own_rows, 0:32, :] = jnp.where(lane < 64, left, scb[own_rows, 0:32, :])
    scb[own_rows, 32:64, :] = jnp.where(
        lane < 32, roll(left, -32), jnp.where(lane < 96, coarse, roll(right, 32))
    )
    scb[own_rows, 64:96, :] = jnp.where(lane < 64, scb[own_rows, 64:96, :], right)
    lane = lane_of((2, 32, 128))
    for k, at in ((0, 0), (3, 10)):
        rows = two(roll(rim[k], 32), roll(rim[k], -32))
        left, right = two(rim[k + 1], roll(rim[k + 1], 64)), two(roll(rim[k + 2], 64), rim[k + 2])
        left = jnp.where(lane < lo64, left, zero(left))
        right = jnp.where(lane >= hi64, right, zero(right))
        scb[at : at + 2, 0:32, :] = jnp.where(lane < 64, left, roll(rows, 32))
        scb[at : at + 2, 32:64, :] = jnp.where(
            lane < 32, roll(left, -32), jnp.where(lane < 96, rows, roll(right, 32))
        )
        scb[at : at + 2, 64:96, :] = jnp.where(lane < 64, roll(rows, -32), right)

    conv_rows(scb, 10, wb_f, 64, lin_b_s)
    lin_b = lin_b_s[...]
    sig_b = sigmoid(lin_b)
    slope_b = sig_b * (1.0 + lin_b * (1.0 - sig_b))
    gated = (lin_b * sig_b)[1:9].astype(BF)
    grad_b = jnp.concatenate(
        [(grad_gated[:, 128 * r : 128 * (r + 1)] * slope_b[r]).astype(BF)[None] for r in range(10)],
        axis=0,
    )
    top, low = grad_b[0:6], grad_b[4:10]
    lane = lane_of(top.shape)
    sgb[:, 0:64, :] = jnp.where(lane < 64, top, roll(low, 64))
    sgb[:, 64:128, :] = pack_pair(top, low)
    sgb[:, 128:192, :] = jnp.where(lane < 64, roll(top, 64), low)

    shifts = layer_shifts(sgb[1:5, 64:128, :])
    up = side_by_side([jnp.concatenate([s[r] for s in shifts], axis=0) for r in range(4)])
    seen = pack_pair(scb[1:7], scb[5:11])
    seen = side_by_side([seen[r : r + 3].reshape(288, 128) for r in range(4)])
    gated = pack_pair(gated[0:4], gated[4:8])
    sum_b = dot_nt(seen, up)
    sum_m = dot_nt(
        side_by_side([fold_pairs[r] for r in range(4)]), side_by_side([gated[r] for r in range(4)])
    )
    for i in range(18):
        pb[i] = sum_b[16 * i : 16 * i + 16, 0:128].astype(BF)
    rest = side_by_side([sum_b[144 * g : 144 * g + 144, 128:192] for g in range(2)])
    for i in range(9):
        pb[18 + i] = rest[16 * i : 16 * i + 16].astype(BF)
    pb[27] = side_by_side([sum_m[0:16], sum_m[16:32]]).astype(BF)
    for t in range(28, PLANE):
        pb[t] = jnp.zeros((16, 128), BF)

    def spread(buf, dst, k):
        for i, step in enumerate(steps):
            q = plane_p[step[0]] * n_eta + eta_of[step[1]]
            send(buf.at[q], dst.at[i], s_send.at[k], s_recv.at[k], plane_device(step))
        copy = whole(dst, s_send.at[k], s_recv.at[k])
        departures.append(copy)
        return copy

    spread_b = spread(pb, rb, 0)

    conv_rows(sgb, 4, wb_b, 32, gc_s)
    grad_coarse = widen_pairs(gc_s[...].astype(BF).astype(F32))
    grad_hidden = jnp.concatenate(
        [(ct[:, i] + 0.25 * grad_coarse)[:, None] for i in range(2)], axis=1
    ).reshape(16, 32, 128)
    grad_a = (grad_hidden * slope_a_s[...]).astype(BF)
    g_s[...] = grad_a
    shifts = layer_shifts(grad_a)
    up = side_by_side([jnp.concatenate([s[r] for s in shifts], axis=0) for r in range(16)])
    sum_a = dot(up, sft[...].reshape(2048, 288))
    for i in range(12):
        for l in range(2):
            pa[2 * i + l] = sum_a[8 * i : 8 * i + 8, 128 * l : 128 * l + 128].astype(BF)
    rest = side_by_side([sum_a[32 * g : 32 * g + 32, 256:288] for g in range(3)])
    rest = jnp.concatenate([rest, jnp.zeros((32, 32), F32)], axis=1)
    for i in range(4):
        pa[24 + i] = rest[8 * i : 8 * i + 8].astype(BF)
    for t in range(28, PLANE):
        pa[t] = jnp.zeros((8, 128), BF)
    spread_a = spread(pa, ra, 1)
    colg_s[0] = pack_column(grad_a, 4, 96)
    colg_s[1] = pack_column(grad_a, 4, 0)
    projected = dot(mix, side_by_side([gated[r] for r in range(4)])).astype(BF).astype(F32)
    projected = jnp.concatenate(
        [projected[:, 128 * r : 128 * (r + 1)][None] for r in range(4)], axis=0
    )
    projected = widen_pairs(projected)
    output = jnp.concatenate(
        [(hidden[:, i] + projected)[:, None] for i in range(2)], axis=1
    ).reshape(16, 32, 128)
    out_ref[...] = jnp.transpose(output.astype(BF), (1, 0, 2))

    def cross(copy, buf, arrived, mine, slots, k):
        copy.wait_recv()
        total = buf[me1].astype(F32)
        for i in range(g1 - 1):
            total = total + arrived[i].astype(F32)
        total = total.astype(BF)
        mine[...] = total
        slots[me2] = total
        for i in range(1, g2):
            send(mine, slots.at[me2], s_send.at[k], s_recv.at[k], line_device(i))
        copy = whole(slots.at[pl.ds(0, g2 - 1)], s_send.at[k], s_recv.at[k])
        departures.append(copy)
        return copy

    def gather(copy, slots, mine, result, k):
        copy.wait_recv()
        total = slots[0].astype(F32)
        for i in range(1, g2):
            total = total + slots[i].astype(F32)
        total = total.astype(BF)
        mine[...] = total
        result[me1] = total
        for step in steps:
            send(mine, result.at[me1], s_send.at[k], s_recv.at[k], plane_device(step))
        copy = whole(result.at[pl.ds(0, g1 - 1)], s_send.at[k], s_recv.at[k])
        departures.append(copy)
        return copy

    cross_b = cross(spread_b, pb, rb, xb2, rb2, 2)
    cross_a = cross(spread_a, pa, ra, xa2, ra2, 3)
    halo_g = halo_start(
        3, (colg_s.at[0], colg_s.at[1]), (g_s.at[15], g_s.at[0]), rg
    )

    gather_b = gather(cross_b, rb2, xb3, resb, 4)
    gather_a = gather(cross_a, ra2, xa3, resa, 5)

    fine_windows_own(sga, grad_a)
    halo_g.wait_recv()
    fine_windows_rim(sga, rg)
    conv_rows(sga, 16, wa_b, 32, gi_s)
    gi_ref[...] = jnp.transpose(gi_s[...].astype(BF), (1, 0, 2))

    gather_b.wait_recv()
    for ab in range(9):
        for h in range(2):
            rows = slice(16 * h, 16 * h + 16)
            u = 2 * ab + h
            pair = resb[u].astype(F32) * scale
            gkb_ref[3 * ab, rows, :] = pair[:, 0:64]
            gkb_ref[3 * ab + 1, rows, :] = pair[:, 64:128]
            g = u // 9
            rest = resb[18 + u % 9].astype(F32) * scale
            gkb_ref[3 * ab + 2, rows, :] = rest[:, 64 * g : 64 * g + 64]
    last = resb[27].astype(F32) * scale
    gm_ref[0:16, :] = last[:, 0:64]
    gm_ref[16:32, :] = last[:, 64:128]

    gather_a.wait_recv()
    for c in range(3):
        for h in range(4):
            rows = slice(8 * h, 8 * h + 8)
            for l in range(2):
                block = resa[2 * (4 * c + h) + l].astype(F32) * scale
                for q in range(4):
                    gka_ref[(4 * l + q) * 3 + c, rows, :] = block[:, 32 * q : 32 * q + 32]
            rest = resa[24 + h].astype(F32) * scale
            gka_ref[24 + c, rows, :] = rest[:, 32 * c : 32 * c + 32]

    for copy in departures:
        copy.wait_send()


def writer(*refs):
    sems = refs[10]
    copies = [
        pltpu.make_async_copy(src, dst, sems.at[k])
        for k, (src, dst) in enumerate(zip(refs[:5], refs[5:10]))
    ]
    for copy in copies:
        copy.start()
    for copy in copies:
        copy.wait()


def shards(n_phi, n_eta, features, cotangent, kernel_a, kernel_b, mixing):
    g1, g2 = 4 * n_eta, n_phi // 4
    assert g1 == PLANE
    cells = features.shape[1] * features.shape[2] * n_phi * n_eta
    kernel_b = jnp.swapaxes(kernel_b, 1, 2)
    ins = (features, cotangent, kernel_a, kernel_b, mixing)
    types = (BF, BF, F32, F32, F32)

    def vm(*shape, dtype=BF):
        return pltpu.VMEM(shape, dtype)

    def sums(n):
        return [
            vm(g1, n, 128), vm(g1 - 1, n, 128), vm(n, 128),
            vm(g2, n, 128), vm(n, 128), vm(g1, n, 128),
        ]

    def halo(n):
        return [vm(2 * n + 6, 32, 128)]

    dma = pltpu.SemaphoreType.DMA
    scratch = [
        *[vm(*a.shape) for a in ins], dma((5,)),
        vm(16, 32, 128), vm(2, 4, 32, 128), *halo(4),
        vm(8, 32, 128), vm(2, 2, 32, 128), *halo(2),
        vm(4, 32, 128), vm(2, 32, 128), *halo(4),
        vm(16, 32, 128), vm(2, 4, 32, 128), *halo(4),
        vm(18, 96, 128), vm(16, 128, 288), vm(12, 96, 128), vm(6, 192, 128), vm(18, 96, 128),
        vm(16, 32, 128, dtype=F32), vm(16, 32, 128, dtype=F32), vm(10, 64, 128, dtype=F32),
        vm(4, 32, 128, dtype=F32), vm(16, 32, 128, dtype=F32),
        *sums(8), *sums(16),
        *[dma((k,)) for k in (4, 4, 6, 6)],
    ]
    vmem = pl.BlockSpec(memory_space=pltpu.VMEM)
    anywhere = pl.BlockSpec(memory_space=pl.ANY)
    shapes = [a.shape for a in ins]
    outs = pl.pallas_call(
        functools.partial(kernel, n_phi, n_eta, 1.0 / math.sqrt(cells)),
        out_shape=tuple(pltpu.VMEM(s, t) for s, t in zip(shapes, types)),
        in_specs=[anywhere] * 5,
        out_specs=(vmem,) * 5,
        scratch_shapes=scratch,
        compiler_params=pltpu.CompilerParams(collective_id=0, has_side_effects=True),
        name="block_step",
    )(*ins)
    outs = pl.pallas_call(
        writer,
        out_shape=tuple(jax.ShapeDtypeStruct(s, t) for s, t in zip(shapes, types)),
        in_specs=[vmem] * 5,
        out_specs=(anywhere,) * 5,
        scratch_shapes=[dma((5,))],
        name="write_out",
    )(*[pltpu.with_memory_space_constraint(o, pltpu.VMEM) for o in outs])
    return (*outs[:3], jnp.swapaxes(outs[3], 1, 2), outs[4])


def solution(mesh):
    specs = (P(None, "phi", "eta"), P(None, "phi", "eta"), P(), P(), P())
    body = functools.partial(shards, mesh.shape["phi"], mesh.shape["eta"])
    return jax.shard_map(body, mesh=mesh, in_specs=specs, out_specs=specs, check_vma=False)
```

```python
import functools
import math

import jax
import jax.numpy as jnp
from jax import lax
from jax.experimental import pallas as pl
from jax.experimental.pallas import tpu as pltpu
from jax.sharding import PartitionSpec as P

BF = jnp.bfloat16
F32 = jnp.float32
MESH = pl.DeviceIdType.MESH
DIRS = ((0, 1), (0, -1), (1, 0), (1, 1), (1, -1), (-1, 0), (-1, 1), (-1, -1))
PLANE = 32


def lane_of(shape):
    return lax.broadcasted_iota(jnp.int32, shape, len(shape) - 1)


def roll(x, shift):
    shift %= 128
    return x if shift == 0 else pltpu.roll(x, shift, x.ndim - 1)


def dot(a, b):
    return jnp.dot(a, b, preferred_element_type=F32)


def dot_nt(a, b):
    return lax.dot_general(a, b, (((1,), (1,)), ((), ())), preferred_element_type=F32)


def zero(x):
    return jnp.zeros((), x.dtype)


def side_by_side(rows):
    return jnp.concatenate(rows, axis=1)


def by_quarter(v0, v1, v2, v3):
    lane = lane_of(v0.shape)
    return jnp.where(
        lane < 64, jnp.where(lane < 32, v0, v1), jnp.where(lane < 96, v2, v3)
    )


def pack_column(x, size, start):
    return by_quarter(
        *[roll(x[size * g : size * (g + 1)], 32 * g - start) for g in range(4)]
    )


def unpack_column(packed, want):
    return [roll(packed, want - 32 * g) for g in range(4)]


def pack_pair(x, y):
    return jnp.where(lane_of(x.shape) < 64, roll(x, -32), roll(y, 32))


def widen_pairs(x):
    up, down, across = roll(x, 32), roll(x, -32), roll(x, 64)
    low, high = by_quarter(x, up, up, across), by_quarter(across, down, down, x)
    return jnp.concatenate([low, high], axis=0)


def pool_columns(x):
    lane = lane_of(x.shape)
    both = x + jnp.where(lane < 64, roll(x, 32), roll(x, -32))
    return jnp.where((lane >= 32) & (lane < 96), both, zero(x))


def layer_shifts(x):
    layer = lane_of(x.shape) % 32
    return [
        jnp.where(layer < 31, roll(x, -1), zero(x)),
        x,
        jnp.where(layer > 0, roll(x, 1), zero(x)),
    ]


def merge_layers(z):
    outs = z.shape[0] // 3
    layer = lane_of((outs, 128)) % 32
    low = jnp.where(layer > 0, roll(z[:outs], 1), 0.0)
    high = jnp.where(layer < 31, roll(z[2 * outs :], -1), 0.0)
    return z[outs : 2 * outs] + low + high


def conv_rows(src, count, weight, outs, sink):
    layer = lane_of((outs, 128)) % 32
    flat = 3 * src.shape[1]
    for r in range(0, count, 2):
        pair = [src[r + i : r + i + 3].reshape(flat, 128) for i in range(2)]
        z = dot(weight, side_by_side(pair))
        for i in range(2):
            zi = z[:, 128 * i : 128 * (i + 1)]
            low = jnp.where(layer > 0, roll(zi[:outs], 1), 0.0)
            high = jnp.where(layer < 31, roll(zi[2 * outs :], -1), 0.0)
            sink[r + i] = zi[outs : 2 * outs] + low + high


def sigmoid(v):
    return 1.0 / (1.0 + jnp.exp(-v))


def kernel(n_phi, n_eta, scale, *refs):
    ins, (out_ref, gi_ref, gka_ref, gkb_ref, gm_ref) = refs[:5], refs[5:10]
    (
        f_ref, ct_ref, ka_ref, kb_ref, mix_ref, load_sem,
        x_s, colx_s, rx,
        fold_s, colf_s, rf,
        colc_s, rowc_s, rc,
        g_s, colg_s, rg,
        sfa, sft, scb, sgb, sga, slope_a_s, lin_a_s, lin_b_s, gc_s, gi_s,
        pa, ra, xa2, ra2, xa3, resa, pb, rb, xb2, rb2, xb3, resb,
        h_send, h_recv, s_send, s_recv,
    ) = refs[10:]
    p = lax.axis_index("phi")
    e = lax.axis_index("eta")
    g1, g2 = 4 * n_eta, n_phi // 4
    me2 = p // 4

    def wrap(i, n):
        return jnp.where(i >= n, i - n, i)

    in_plane = lax.rem(p, 4)
    plane_p = [wrap(in_plane + i, 4) for i in range(4)]
    phi_of = [me2 * 4 + i for i in plane_p]
    eta_of = [wrap(e + i, n_eta) for i in range(n_eta)]
    line_of = [wrap(p + 4 * i, n_phi) for i in range(g2)]
    near_of = {0: p, 1: wrap(p + 1, n_phi), -1: wrap(p + n_phi - 1, n_phi)}
    me1 = in_plane * n_eta + e
    steps = [(i, j) for i in range(4) for j in range(n_eta) if i or j]
    steps.sort(key=lambda ij: (-min(ij[1], n_eta - ij[1]), -min(ij[0], 4 - ij[0])))

    def halo_device(d):
        return (near_of[d[0]], eta_of[d[1] % n_eta])

    def plane_device(step):
        return (phi_of[step[0]], eta_of[step[1]])

    def line_device(i):
        return (line_of[i], e)

    loads = [
        pltpu.make_async_copy(src, dst, load_sem.at[k])
        for k, (src, dst) in enumerate(zip(ins, (f_ref, ct_ref, ka_ref, kb_ref, mix_ref)))
    ]
    loads[0].start()

    barrier = pltpu.get_barrier_semaphore()
    targets = [line_device(i) for i in sorted(range(1, g2), key=lambda i: -min(i, g2 - i))]
    planes = [plane_device(step) for step in steps]
    targets += planes[:12] + [halo_device(d) for d in DIRS] + planes[12:]
    for target in targets:
        pl.semaphore_signal(barrier, inc=1, device_id=target, device_id_type=MESH)
    for load in loads[1:]:
        load.start()

    departures = []

    def send(src, dst, ssem, rsem, target):
        pltpu.make_async_remote_copy(
            src_ref=src, dst_ref=dst, send_sem=ssem, recv_sem=rsem,
            device_id=target, device_id_type=MESH,
        ).start()

    def whole(ref, ssem, rsem):
        return pltpu.make_async_remote_copy(
            src_ref=ref, dst_ref=ref, send_sem=ssem, recv_sem=rsem,
            device_id=(p, e), device_id_type=MESH,
        )

    def halo_start(which, cols, rows, arrived):
        n = (arrived.shape[0] - 6) // 2
        ssem, rsem = h_send.at[which], h_recv.at[which]
        for k, d in sorted(enumerate(DIRS), key=lambda kd: -abs(kd[1][0]) - abs(kd[1][1])):
            if k < 2:
                src, dst = cols[k], arrived.at[pl.ds(n * k, n)]
            else:
                src, dst = rows[0 if d[0] > 0 else 1], arrived.at[2 * n + k - 2]
            send(src, dst, ssem, rsem, halo_device(d))
        copy = whole(arrived, ssem, rsem)
        departures.append(copy)
        return copy

    def halo_parts(arrived):
        n = (arrived.shape[0] - 6) // 2
        rows = [arrived[2 * n + j : 2 * n + j + 1] for j in range(6)]
        return (arrived[0:n], arrived[n : 2 * n]), rows

    has_left = e > 0
    has_right = e < n_eta - 1
    lo32 = jnp.where(has_left, 32, 0)
    lo64 = jnp.where(has_left, 64, 0)
    hi96 = jnp.where(has_right, 96, 128)
    hi64 = jnp.where(has_right, 64, 128)

    loads[0].wait()
    x = jnp.transpose(f_ref[...], (1, 0, 2))
    x_s[...] = x
    colx_s[0] = pack_column(x, 4, 96)
    colx_s[1] = pack_column(x, 4, 0)
    pl.semaphore_wait(barrier, len(targets))
    halo_x = halo_start(
        0, (colx_s.at[0], colx_s.at[1]), (x_s.at[15], x_s.at[0]), rx
    )

    for load in loads[1:]:
        load.wait()
    ct = jnp.transpose(ct_ref[...], (1, 0, 2)).astype(F32).reshape(8, 2, 32, 128)
    fold = pool_columns(ct[:, 0] + ct[:, 1]).astype(BF)
    fold_s[...] = fold
    colf_s[0] = pack_column(fold, 2, 64)
    colf_s[1] = pack_column(fold, 2, 32)

    def forward_weight(ref):
        return jnp.concatenate(
            [side_by_side([ref[3 * ab + c] for ab in range(9)]) for c in range(3)], axis=0
        )

    def backward_weight(ref):
        return jnp.concatenate(
            [side_by_side([ref[26 - 3 * ab - c] for c in range(3)]) for ab in range(9)], axis=0
        ).T

    wa_f, wa_b = forward_weight(ka_ref), backward_weight(ka_ref)
    wb_f = jnp.concatenate(
        [side_by_side([kb_ref[3 * ab + c] for c in range(3)]) for ab in range(9)], axis=0
    ).T
    wb_b = jnp.concatenate(
        [side_by_side([kb_ref[26 - 3 * ab - c] for ab in range(9)]) for c in range(3)], axis=0
    )
    mix = mix_ref[...]
    mix_t = mix.T

    def fine_windows_own(dst, rows):
        lane = lane_of(rows.shape)
        dst[1:17, 0:32, :] = jnp.where(lane < 32, zero(rows), roll(rows, 32))
        dst[1:17, 32:64, :] = rows
        dst[1:17, 64:96, :] = jnp.where(lane >= 96, zero(rows), roll(rows, -32))

    def fine_windows_cols(dst, arrived):
        cols, _ = halo_parts(arrived)
        lane = lane_of((16, 32, 128))
        left = jnp.concatenate(unpack_column(cols[0], 0), axis=0)
        right = jnp.concatenate(unpack_column(cols[1], 96), axis=0)
        dst[1:17, 0:32, :] = jnp.where(lane < lo32, left, dst[1:17, 0:32, :])
        dst[1:17, 64:96, :] = jnp.where(lane >= hi96, right, dst[1:17, 64:96, :])

    def fine_windows_rows(dst, arrived):
        _, rim = halo_parts(arrived)
        lane = lane_of((1, 32, 128))
        for k, at in ((0, 0), (3, 17)):
            rows, left, right = rim[k], roll(rim[k + 1], 32), roll(rim[k + 2], 96)
            dst[at : at + 1, 0:32, :] = jnp.where(
                lane < lo32, left, jnp.where(lane < 32, zero(rows), roll(rows, 32))
            )
            dst[at : at + 1, 32:64, :] = rows
            dst[at : at + 1, 64:96, :] = jnp.where(
                lane >= hi96, right, jnp.where(lane >= 96, zero(rows), roll(rows, -32))
            )

    w_left, w_right = [
        side_by_side([wa_f[:, 96 * a + 32 * b : 96 * a + 32 * b + 32] for a in range(3)])
        for b in (0, 2)
    ]
    w_above, w_below = wa_f[:, 0:96], wa_f[:, 192:288]
    sfa[0] = jnp.zeros((96, 128), BF)
    sfa[17] = jnp.zeros((96, 128), BF)
    fine_windows_own(sfa, x)
    conv_rows(sfa, 16, wa_f, 32, lin_a_s)

    halo_x.wait_send()
    departures.remove(halo_x)
    halo_f = halo_start(
        1, (colf_s.at[0], colf_s.at[1]), (fold_s.at[7], fold_s.at[0]), rf
    )
    halo_x.wait_recv()

    def side(packed, weight):
        lane = lane_of((1, 32, 128))
        before = jnp.where(lane >= 32, roll(packed[3:4], 32), zero(packed))
        after = jnp.where(lane < 96, roll(packed[0:1], -32), zero(packed))
        rows = jnp.concatenate([before, packed, after], axis=0)
        z = dot(weight, side_by_side([rows[q : q + 3].reshape(96, 128) for q in range(4)]))
        return jnp.concatenate(
            [merge_layers(z[:, 128 * q : 128 * q + 128])[None] for q in range(4)], axis=0
        )

    cols, _ = halo_parts(rx)
    left = jnp.concatenate(unpack_column(side(cols[0], w_left), 0), axis=0)
    right = jnp.concatenate(unpack_column(side(cols[1], w_right), 96), axis=0)
    lane = lane_of((16, 32, 128))
    lin_a_s[...] += jnp.where(lane < lo32, left, jnp.where(lane >= hi96, right, 0.0))
    fine_windows_rows(sfa, rx)
    lin_a_s[0] += merge_layers(dot(w_above, sfa[0]))
    lin_a_s[15] += merge_layers(dot(w_below, sfa[17]))
    lin_a = lin_a_s[...]
    hidden = (lin_a / (1.0 + jnp.exp(-lin_a))).astype(BF).astype(F32).reshape(8, 2, 32, 128)
    coarse = (0.25 * pool_columns(hidden[:, 0] + hidden[:, 1])).astype(BF)

    colc_s[...] = pack_pair(coarse[0:4], coarse[4:8])
    rowc_s[0:1] = pack_pair(coarse[6:7], coarse[7:8])
    rowc_s[1:2] = pack_pair(coarse[0:1], coarse[1:2])
    halo_c = halo_start(2, (colc_s, colc_s), (rowc_s.at[0], rowc_s.at[1]), rc)

    halo_f.wait_recv()
    cols, rim = halo_parts(rf)
    fold_rows = jnp.concatenate([rim[0], fold, rim[3]], axis=0)
    fold_left = jnp.concatenate(
        [roll(rim[1], 64)] + unpack_column(cols[0], 0) + [roll(rim[4], 64)], axis=0
    )
    fold_right = jnp.concatenate(
        [roll(rim[2], 64)] + unpack_column(cols[1], 96) + [roll(rim[5], 64)], axis=0
    )
    lane = lane_of(fold_rows.shape)
    fold_wide = jnp.where(
        (lane >= 32) & (lane < 96),
        fold_rows,
        jnp.where(
            lane < lo32, fold_left, jnp.where(lane >= hi96, fold_right, zero(fold_rows))
        ),
    )

    fold_pairs = pack_pair(fold[0:4], fold[4:8])
    grad_gated = dot(mix_t, side_by_side([fold_wide[r] for r in range(10)]))
    sig_a = sigmoid(lin_a)
    slope_a_s[...] = sig_a * (1.0 + lin_a * (1.0 - sig_a))

    own_rows = slice(2, 10)
    lane = lane_of(coarse.shape)
    scb[own_rows, 0:32, :] = jnp.where(lane < 64, zero(coarse), roll(coarse, 32))
    scb[own_rows, 32:64, :] = coarse
    scb[own_rows, 64:96, :] = jnp.where(lane < 64, roll(coarse, -32), zero(coarse))

    fine_windows_cols(sfa, rx)
    for r in range(16):
        sft[r] = sfa[r : r + 3].reshape(288, 128).T

    halo_c.wait_recv()
    cols, rim = halo_parts(rc)

    def two(*parts):
        return jnp.concatenate(parts, axis=0)

    left, right = two(cols[0], roll(cols[0], 64)), two(roll(cols[1], 64), cols[1])
    left = jnp.where(lane < lo64, left, zero(left))
    right = jnp.where(lane >= hi64, right, zero(right))
    scb[own_rows, 0:32, :] = jnp.where(lane < 64, left, scb[own_rows, 0:32, :])
    scb[own_rows, 32:64, :] = jnp.where(
        lane < 32, roll(left, -32), jnp.where(lane < 96, coarse, roll(right, 32))
    )
    scb[own_rows, 64:96, :] = jnp.where(lane < 64, scb[own_rows, 64:96, :], right)
    lane = lane_of((2, 32, 128))
    for k, at in ((0, 0), (3, 10)):
        rows = two(roll(rim[k], 32), roll(rim[k], -32))
        left, right = two(rim[k + 1], roll(rim[k + 1], 64)), two(roll(rim[k + 2], 64), rim[k + 2])
        left = jnp.where(lane < lo64, left, zero(left))
        right = jnp.where(lane >= hi64, right, zero(right))
        scb[at : at + 2, 0:32, :] = jnp.where(lane < 64, left, roll(rows, 32))
        scb[at : at + 2, 32:64, :] = jnp.where(
            lane < 32, roll(left, -32), jnp.where(lane < 96, rows, roll(right, 32))
        )
        scb[at : at + 2, 64:96, :] = jnp.where(lane < 64, roll(rows, -32), right)

    conv_rows(scb, 10, wb_f, 64, lin_b_s)
    lin_b = lin_b_s[...]
    sig_b = sigmoid(lin_b)
    slope_b = sig_b * (1.0 + lin_b * (1.0 - sig_b))
    gated = (lin_b * sig_b)[1:9].astype(BF)
    grad_b = jnp.concatenate(
        [(grad_gated[:, 128 * r : 128 * (r + 1)] * slope_b[r]).astype(BF)[None] for r in range(10)],
        axis=0,
    )
    top, low = grad_b[0:6], grad_b[4:10]
    lane = lane_of(top.shape)
    sgb[:, 0:64, :] = jnp.where(lane < 64, top, roll(low, 64))
    sgb[:, 64:128, :] = pack_pair(top, low)
    sgb[:, 128:192, :] = jnp.where(lane < 64, roll(top, 64), low)

    shifts = layer_shifts(sgb[1:5, 64:128, :])
    up = side_by_side([jnp.concatenate([s[r] for s in shifts], axis=0) for r in range(4)])
    seen = pack_pair(scb[1:7], scb[5:11])
    seen = side_by_side([seen[r : r + 3].reshape(288, 128) for r in range(4)])
    gated = pack_pair(gated[0:4], gated[4:8])
    sum_b = dot_nt(seen, up)
    sum_m = dot_nt(
        side_by_side([fold_pairs[r] for r in range(4)]), side_by_side([gated[r] for r in range(4)])
    )
    for i in range(18):
        pb[i] = sum_b[16 * i : 16 * i + 16, 0:128].astype(BF)
    rest = side_by_side([sum_b[144 * g : 144 * g + 144, 128:192] for g in range(2)])
    for i in range(9):
        pb[18 + i] = rest[16 * i : 16 * i + 16].astype(BF)
    pb[27] = side_by_side([sum_m[0:16], sum_m[16:32]]).astype(BF)
    for t in range(28, PLANE):
        pb[t] = jnp.zeros((16, 128), BF)

    def spread(buf, dst, k):
        for i, step in enumerate(steps):
            q = plane_p[step[0]] * n_eta + eta_of[step[1]]
            send(buf.at[q], dst.at[i], s_send.at[k], s_recv.at[k], plane_device(step))
        copy = whole(dst, s_send.at[k], s_recv.at[k])
        departures.append(copy)
        return copy

    spread_b = spread(pb, rb, 0)

    conv_rows(sgb, 4, wb_b, 32, gc_s)
    grad_coarse = widen_pairs(gc_s[...].astype(BF).astype(F32))
    grad_hidden = jnp.concatenate(
        [(ct[:, i] + 0.25 * grad_coarse)[:, None] for i in range(2)], axis=1
    ).reshape(16, 32, 128)
    grad_a = (grad_hidden * slope_a_s[...]).astype(BF)
    g_s[...] = grad_a
    shifts = layer_shifts(grad_a)
    up = side_by_side([jnp.concatenate([s[r] for s in shifts], axis=0) for r in range(16)])
    sum_a = dot(up, sft[...].reshape(2048, 288))
    for i in range(12):
        for l in range(2):
            pa[2 * i + l] = sum_a[8 * i : 8 * i + 8, 128 * l : 128 * l + 128].astype(BF)
    rest = side_by_side([sum_a[32 * g : 32 * g + 32, 256:288] for g in range(3)])
    rest = jnp.concatenate([rest, jnp.zeros((32, 32), F32)], axis=1)
    for i in range(4):
        pa[24 + i] = rest[8 * i : 8 * i + 8].astype(BF)
    for t in range(28, PLANE):
        pa[t] = jnp.zeros((8, 128), BF)
    spread_a = spread(pa, ra, 1)
    colg_s[0] = pack_column(grad_a, 4, 96)
    colg_s[1] = pack_column(grad_a, 4, 0)
    projected = dot(mix, side_by_side([gated[r] for r in range(4)])).astype(BF).astype(F32)
    projected = jnp.concatenate(
        [projected[:, 128 * r : 128 * (r + 1)][None] for r in range(4)], axis=0
    )
    projected = widen_pairs(projected)
    output = jnp.concatenate(
        [(hidden[:, i] + projected)[:, None] for i in range(2)], axis=1
    ).reshape(16, 32, 128)
    out_ref[...] = jnp.transpose(output.astype(BF), (1, 0, 2))

    def cross(copy, buf, arrived, mine, slots, k):
        copy.wait_recv()
        total = buf[me1].astype(F32)
        for i in range(g1 - 1):
            total = total + arrived[i].astype(F32)
        total = total.astype(BF)
        mine[...] = total
        slots[me2] = total
        for i in range(1, g2):
            send(mine, slots.at[me2], s_send.at[k], s_recv.at[k], line_device(i))
        copy = whole(slots.at[pl.ds(0, g2 - 1)], s_send.at[k], s_recv.at[k])
        departures.append(copy)
        return copy

    def gather(copy, slots, mine, result, k):
        copy.wait_recv()
        total = slots[0].astype(F32)
        for i in range(1, g2):
            total = total + slots[i].astype(F32)
        total = total.astype(BF)
        mine[...] = total
        result[me1] = total
        for step in steps:
            send(mine, result.at[me1], s_send.at[k], s_recv.at[k], plane_device(step))
        copy = whole(result.at[pl.ds(0, g1 - 1)], s_send.at[k], s_recv.at[k])
        departures.append(copy)
        return copy

    cross_b = cross(spread_b, pb, rb, xb2, rb2, 2)
    cross_a = cross(spread_a, pa, ra, xa2, ra2, 3)
    halo_g = halo_start(
        3, (colg_s.at[0], colg_s.at[1]), (g_s.at[15], g_s.at[0]), rg
    )

    gather_b = gather(cross_b, rb2, xb3, resb, 4)
    gather_a = gather(cross_a, ra2, xa3, resa, 5)

    fine_windows_own(sga, grad_a)
    halo_g.wait_recv()
    fine_windows_cols(sga, rg)
    fine_windows_rows(sga, rg)
    conv_rows(sga, 16, wa_b, 32, gi_s)
    gi_ref[...] = jnp.transpose(gi_s[...].astype(BF), (1, 0, 2))

    gather_b.wait_recv()
    for ab in range(9):
        for h in range(2):
            rows = slice(16 * h, 16 * h + 16)
            u = 2 * ab + h
            pair = resb[u].astype(F32) * scale
            gkb_ref[3 * ab, rows, :] = pair[:, 0:64]
            gkb_ref[3 * ab + 1, rows, :] = pair[:, 64:128]
            g = u // 9
            rest = resb[18 + u % 9].astype(F32) * scale
            gkb_ref[3 * ab + 2, rows, :] = rest[:, 64 * g : 64 * g + 64]
    last = resb[27].astype(F32) * scale
    gm_ref[0:16, :] = last[:, 0:64]
    gm_ref[16:32, :] = last[:, 64:128]

    gather_a.wait_recv()
    for c in range(3):
        for h in range(4):
            rows = slice(8 * h, 8 * h + 8)
            for l in range(2):
                block = resa[2 * (4 * c + h) + l].astype(F32) * scale
                for q in range(4):
                    gka_ref[(4 * l + q) * 3 + c, rows, :] = block[:, 32 * q : 32 * q + 32]
            rest = resa[24 + h].astype(F32) * scale
            gka_ref[24 + c, rows, :] = rest[:, 32 * c : 32 * c + 32]

    for copy in departures:
        copy.wait_send()


def writer(*refs):
    sems = refs[10]
    copies = [
        pltpu.make_async_copy(src, dst, sems.at[k])
        for k, (src, dst) in enumerate(zip(refs[:5], refs[5:10]))
    ]
    for copy in copies:
        copy.start()
    for copy in copies:
        copy.wait()


def shards(n_phi, n_eta, features, cotangent, kernel_a, kernel_b, mixing):
    g1, g2 = 4 * n_eta, n_phi // 4
    assert g1 == PLANE
    cells = features.shape[1] * features.shape[2] * n_phi * n_eta
    kernel_b = jnp.swapaxes(kernel_b, 1, 2)
    ins = (features, cotangent, kernel_a, kernel_b, mixing)
    types = (BF, BF, F32, F32, F32)

    def vm(*shape, dtype=BF):
        return pltpu.VMEM(shape, dtype)

    def sums(n):
        return [
            vm(g1, n, 128), vm(g1 - 1, n, 128), vm(n, 128),
            vm(g2, n, 128), vm(n, 128), vm(g1, n, 128),
        ]

    def halo(n):
        return [vm(2 * n + 6, 32, 128)]

    dma = pltpu.SemaphoreType.DMA
    scratch = [
        *[vm(*a.shape) for a in ins], dma((5,)),
        vm(16, 32, 128), vm(2, 4, 32, 128), *halo(4),
        vm(8, 32, 128), vm(2, 2, 32, 128), *halo(2),
        vm(4, 32, 128), vm(2, 32, 128), *halo(4),
        vm(16, 32, 128), vm(2, 4, 32, 128), *halo(4),
        vm(18, 96, 128), vm(16, 128, 288), vm(12, 96, 128), vm(6, 192, 128), vm(18, 96, 128),
        vm(16, 32, 128, dtype=F32), vm(16, 32, 128, dtype=F32), vm(10, 64, 128, dtype=F32),
        vm(4, 32, 128, dtype=F32), vm(16, 32, 128, dtype=F32),
        *sums(8), *sums(16),
        *[dma((k,)) for k in (4, 4, 6, 6)],
    ]
    vmem = pl.BlockSpec(memory_space=pltpu.VMEM)
    anywhere = pl.BlockSpec(memory_space=pl.ANY)
    shapes = [a.shape for a in ins]
    outs = pl.pallas_call(
        functools.partial(kernel, n_phi, n_eta, 1.0 / math.sqrt(cells)),
        out_shape=tuple(pltpu.VMEM(s, t) for s, t in zip(shapes, types)),
        in_specs=[anywhere] * 5,
        out_specs=(vmem,) * 5,
        scratch_shapes=scratch,
        compiler_params=pltpu.CompilerParams(collective_id=0, has_side_effects=True),
        name="block_step",
    )(*ins)
    outs = pl.pallas_call(
        writer,
        out_shape=tuple(jax.ShapeDtypeStruct(s, t) for s, t in zip(shapes, types)),
        in_specs=[vmem] * 5,
        out_specs=(anywhere,) * 5,
        scratch_shapes=[dma((5,))],
        name="write_out",
    )(*[pltpu.with_memory_space_constraint(o, pltpu.VMEM) for o in outs])
    return (*outs[:3], jnp.swapaxes(outs[3], 1, 2), outs[4])


def solution(mesh):
    specs = (P(None, "phi", "eta"), P(None, "phi", "eta"), P(), P(), P())
    body = functools.partial(shards, mesh.shape["phi"], mesh.shape["eta"])
    return jax.shard_map(body, mesh=mesh, in_specs=specs, out_specs=specs, check_vma=False)
```

```python
import functools
import math

import jax
import jax.numpy as jnp
from jax import lax
from jax.experimental import pallas as pl
from jax.experimental.pallas import tpu as pltpu
from jax.sharding import PartitionSpec as P

BF = jnp.bfloat16
F32 = jnp.float32
MESH = pl.DeviceIdType.MESH
DIRS = ((0, 1), (0, -1), (1, 0), (1, 1), (1, -1), (-1, 0), (-1, 1), (-1, -1))
PLANE = 32


def lane_of(shape):
    return lax.broadcasted_iota(jnp.int32, shape, len(shape) - 1)


def roll(x, shift):
    shift %= 128
    return x if shift == 0 else pltpu.roll(x, shift, x.ndim - 1)


def dot(a, b):
    return jnp.dot(a, b, preferred_element_type=F32)


def dot_nt(a, b):
    return lax.dot_general(a, b, (((1,), (1,)), ((), ())), preferred_element_type=F32)


def zero(x):
    return jnp.zeros((), x.dtype)


def side_by_side(rows):
    return jnp.concatenate(rows, axis=1)


def by_quarter(v0, v1, v2, v3):
    lane = lane_of(v0.shape)
    return jnp.where(
        lane < 64, jnp.where(lane < 32, v0, v1), jnp.where(lane < 96, v2, v3)
    )


def pack_column(x, size, start):
    return by_quarter(
        *[roll(x[size * g : size * (g + 1)], 32 * g - start) for g in range(4)]
    )


def unpack_column(packed, want):
    return [roll(packed, want - 32 * g) for g in range(4)]


def pack_pair(x, y):
    return jnp.where(lane_of(x.shape) < 64, roll(x, -32), roll(y, 32))


def widen_pairs(x):
    up, down, across = roll(x, 32), roll(x, -32), roll(x, 64)
    low, high = by_quarter(x, up, up, across), by_quarter(across, down, down, x)
    return jnp.concatenate([low, high], axis=0)


def pool_columns(x):
    lane = lane_of(x.shape)
    both = x + jnp.where(lane < 64, roll(x, 32), roll(x, -32))
    return jnp.where((lane >= 32) & (lane < 96), both, zero(x))


def layer_shifts(x):
    layer = lane_of(x.shape) % 32
    return [
        jnp.where(layer < 31, roll(x, -1), zero(x)),
        x,
        jnp.where(layer > 0, roll(x, 1), zero(x)),
    ]


def merge_layers(z):
    outs = z.shape[0] // 3
    layer = lane_of((outs, 128)) % 32
    low = jnp.where(layer > 0, roll(z[:outs], 1), 0.0)
    high = jnp.where(layer < 31, roll(z[2 * outs :], -1), 0.0)
    return z[outs : 2 * outs] + low + high


def conv_rows(src, count, weight, outs, sink):
    layer = lane_of((outs, 128)) % 32
    flat = 3 * src.shape[1]
    for r in range(0, count, 2):
        pair = [src[r + i : r + i + 3].reshape(flat, 128) for i in range(2)]
        z = dot(weight, side_by_side(pair))
        for i in range(2):
            zi = z[:, 128 * i : 128 * (i + 1)]
            low = jnp.where(layer > 0, roll(zi[:outs], 1), 0.0)
            high = jnp.where(layer < 31, roll(zi[2 * outs :], -1), 0.0)
            sink[r + i] = zi[outs : 2 * outs] + low + high


def sigmoid(v):
    return 1.0 / (1.0 + jnp.exp(-v))


def kernel(n_phi, n_eta, scale, *refs):
    ins, (out_ref, gi_ref, gka_ref, gkb_ref, gm_ref) = refs[:5], refs[5:10]
    (
        f_ref, ct_ref, ka_ref, kb_ref, mix_ref, load_sem,
        x_s, colx_s, rx,
        fold_s, colf_s, rf,
        colc_s, rowc_s, rc,
        g_s, colg_s, rg,
        sfa, sft, scb, sgb, sga, slope_a_s, lin_a_s, lin_b_s, gc_s, gi_s,
        pa, ra, xa2, ra2, xa3, resa, pb, rb, xb2, rb2, xb3, resb,
        h_send, h_recv, s_send, s_recv,
    ) = refs[10:]
    p = lax.axis_index("phi")
    e = lax.axis_index("eta")
    g1, g2 = 4 * n_eta, n_phi // 4
    me2 = p // 4

    def wrap(i, n):
        return jnp.where(i >= n, i - n, i)

    in_plane = lax.rem(p, 4)
    plane_p = [wrap(in_plane + i, 4) for i in range(4)]
    phi_of = [me2 * 4 + i for i in plane_p]
    eta_of = [wrap(e + i, n_eta) for i in range(n_eta)]
    line_of = [wrap(p + 4 * i, n_phi) for i in range(g2)]
    near_of = {0: p, 1: wrap(p + 1, n_phi), -1: wrap(p + n_phi - 1, n_phi)}
    me1 = in_plane * n_eta + e
    steps = [(i, j) for i in range(4) for j in range(n_eta) if i or j]
    steps.sort(key=lambda ij: (-min(ij[1], n_eta - ij[1]), -min(ij[0], 4 - ij[0])))

    def halo_device(d):
        return (near_of[d[0]], eta_of[d[1] % n_eta])

    def plane_device(step):
        return (phi_of[step[0]], eta_of[step[1]])

    def line_device(i):
        return (line_of[i], e)

    loads = [
        pltpu.make_async_copy(src, dst, load_sem.at[k])
        for k, (src, dst) in enumerate(zip(ins, (f_ref, ct_ref, ka_ref, kb_ref, mix_ref)))
    ]
    loads[0].start()

    barrier = pltpu.get_barrier_semaphore()
    targets = [line_device(i) for i in sorted(range(1, g2), key=lambda i: -min(i, g2 - i))]
    planes = [plane_device(step) for step in steps]
    targets += planes[:12] + [halo_device(d) for d in DIRS] + planes[12:]
    for target in targets:
        pl.semaphore_signal(barrier, inc=1, device_id=target, device_id_type=MESH)
    for load in loads[1:]:
        load.start()

    departures = []

    def send(src, dst, ssem, rsem, target):
        pltpu.make_async_remote_copy(
            src_ref=src, dst_ref=dst, send_sem=ssem, recv_sem=rsem,
            device_id=target, device_id_type=MESH,
        ).start()

    def whole(ref, ssem, rsem):
        return pltpu.make_async_remote_copy(
            src_ref=ref, dst_ref=ref, send_sem=ssem, recv_sem=rsem,
            device_id=(p, e), device_id_type=MESH,
        )

    def halo_start(which, cols, rows, arrived):
        n = (arrived.shape[0] - 6) // 2
        ssem, rsem = h_send.at[which], h_recv.at[which]
        for k, d in sorted(enumerate(DIRS), key=lambda kd: -abs(kd[1][0]) - abs(kd[1][1])):
            if k < 2:
                src, dst = cols[k], arrived.at[pl.ds(n * k, n)]
            else:
                src, dst = rows[0 if d[0] > 0 else 1], arrived.at[2 * n + k - 2]
            send(src, dst, ssem, rsem, halo_device(d))
        copy = whole(arrived, ssem, rsem)
        departures.append(copy)
        return copy

    def halo_parts(arrived):
        n = (arrived.shape[0] - 6) // 2
        rows = [arrived[2 * n + j : 2 * n + j + 1] for j in range(6)]
        return (arrived[0:n], arrived[n : 2 * n]), rows

    has_left = e > 0
    has_right = e < n_eta - 1
    lo32 = jnp.where(has_left, 32, 0)
    lo64 = jnp.where(has_left, 64, 0)
    hi96 = jnp.where(has_right, 96, 128)
    hi64 = jnp.where(has_right, 64, 128)

    loads[0].wait()
    x = jnp.transpose(f_ref[...], (1, 0, 2))
    x_s[...] = x
    colx_s[0] = pack_column(x, 4, 96)
    colx_s[1] = pack_column(x, 4, 0)
    pl.semaphore_wait(barrier, len(targets))
    halo_x = halo_start(
        0, (colx_s.at[0], colx_s.at[1]), (x_s.at[15], x_s.at[0]), rx
    )

    for load in loads[1:]:
        load.wait()
    ct = jnp.transpose(ct_ref[...], (1, 0, 2)).astype(F32).reshape(8, 2, 32, 128)
    fold = pool_columns(ct[:, 0] + ct[:, 1]).astype(BF)
    fold_s[...] = fold
    colf_s[0] = pack_column(fold, 2, 64)
    colf_s[1] = pack_column(fold, 2, 32)

    def forward_weight(ref):
        return jnp.concatenate(
            [side_by_side([ref[3 * ab + c] for ab in range(9)]) for c in range(3)], axis=0
        )

    def backward_weight(ref):
        return jnp.concatenate(
            [side_by_side([ref[26 - 3 * ab - c] for c in range(3)]) for ab in range(9)], axis=0
        ).T

    wa_f, wa_b = forward_weight(ka_ref), backward_weight(ka_ref)
    wb_f = jnp.concatenate(
        [side_by_side([kb_ref[3 * ab + c] for c in range(3)]) for ab in range(9)], axis=0
    ).T
    wb_b = jnp.concatenate(
        [side_by_side([kb_ref[26 - 3 * ab - c] for ab in range(9)]) for c in range(3)], axis=0
    )
    mix = mix_ref[...]
    mix_t = mix.T

    def fine_windows_own(dst, rows):
        lane = lane_of(rows.shape)
        dst[1:17, 0:32, :] = jnp.where(lane < 32, zero(rows), roll(rows, 32))
        dst[1:17, 32:64, :] = rows
        dst[1:17, 64:96, :] = jnp.where(lane >= 96, zero(rows), roll(rows, -32))

    def fine_windows_cols(dst, arrived):
        cols, _ = halo_parts(arrived)
        lane = lane_of((16, 32, 128))
        left = jnp.concatenate(unpack_column(cols[0], 0), axis=0)
        right = jnp.concatenate(unpack_column(cols[1], 96), axis=0)
        dst[1:17, 0:32, :] = jnp.where(lane < lo32, left, dst[1:17, 0:32, :])
        dst[1:17, 64:96, :] = jnp.where(lane >= hi96, right, dst[1:17, 64:96, :])

    def fine_windows_rows(dst, arrived):
        _, rim = halo_parts(arrived)
        lane = lane_of((1, 32, 128))
        for k, at in ((0, 0), (3, 17)):
            rows, left, right = rim[k], roll(rim[k + 1], 32), roll(rim[k + 2], 96)
            dst[at : at + 1, 0:32, :] = jnp.where(
                lane < lo32, left, jnp.where(lane < 32, zero(rows), roll(rows, 32))
            )
            dst[at : at + 1, 32:64, :] = rows
            dst[at : at + 1, 64:96, :] = jnp.where(
                lane >= hi96, right, jnp.where(lane >= 96, zero(rows), roll(rows, -32))
            )

    w_left, w_right = [
        side_by_side([wa_f[:, 96 * a + 32 * b : 96 * a + 32 * b + 32] for a in range(3)])
        for b in (0, 2)
    ]
    w_above, w_below = wa_f[:, 0:96], wa_f[:, 192:288]
    sfa[0] = jnp.zeros((96, 128), BF)
    sfa[17] = jnp.zeros((96, 128), BF)
    for t in range(28, PLANE):
        pa[t] = jnp.zeros((8, 128), BF)
        pb[t] = jnp.zeros((16, 128), BF)
    fine_windows_own(sfa, x)
    conv_rows(sfa, 16, wa_f, 32, lin_a_s)

    halo_x.wait_send()
    departures.remove(halo_x)
    halo_f = halo_start(
        1, (colf_s.at[0], colf_s.at[1]), (fold_s.at[7], fold_s.at[0]), rf
    )
    halo_x.wait_recv()

    def side(packed, weight):
        lane = lane_of((1, 32, 128))
        before = jnp.where(lane >= 32, roll(packed[3:4], 32), zero(packed))
        after = jnp.where(lane < 96, roll(packed[0:1], -32), zero(packed))
        rows = jnp.concatenate([before, packed, after], axis=0)
        z = dot(weight, side_by_side([rows[q : q + 3].reshape(96, 128) for q in range(4)]))
        return jnp.concatenate(
            [merge_layers(z[:, 128 * q : 128 * q + 128])[None] for q in range(4)], axis=0
        )

    cols, _ = halo_parts(rx)
    left = jnp.concatenate(unpack_column(side(cols[0], w_left), 0), axis=0)
    right = jnp.concatenate(unpack_column(side(cols[1], w_right), 96), axis=0)
    lane = lane_of((16, 32, 128))
    lin_a_s[...] += jnp.where(lane < lo32, left, jnp.where(lane >= hi96, right, 0.0))
    fine_windows_rows(sfa, rx)
    lin_a_s[0] += merge_layers(dot(w_above, sfa[0]))
    lin_a_s[15] += merge_layers(dot(w_below, sfa[17]))
    lin_a = lin_a_s[...]
    hidden = (lin_a / (1.0 + jnp.exp(-lin_a))).astype(BF).astype(F32).reshape(8, 2, 32, 128)
    coarse = (0.25 * pool_columns(hidden[:, 0] + hidden[:, 1])).astype(BF)

    colc_s[...] = pack_pair(coarse[0:4], coarse[4:8])
    rowc_s[0:1] = pack_pair(coarse[6:7], coarse[7:8])
    rowc_s[1:2] = pack_pair(coarse[0:1], coarse[1:2])
    halo_c = halo_start(2, (colc_s, colc_s), (rowc_s.at[0], rowc_s.at[1]), rc)

    halo_f.wait_recv()
    cols, rim = halo_parts(rf)
    fold_rows = jnp.concatenate([rim[0], fold, rim[3]], axis=0)
    fold_left = jnp.concatenate(
        [roll(rim[1], 64)] + unpack_column(cols[0], 0) + [roll(rim[4], 64)], axis=0
    )
    fold_right = jnp.concatenate(
        [roll(rim[2], 64)] + unpack_column(cols[1], 96) + [roll(rim[5], 64)], axis=0
    )
    lane = lane_of(fold_rows.shape)
    fold_wide = jnp.where(
        (lane >= 32) & (lane < 96),
        fold_rows,
        jnp.where(
            lane < lo32, fold_left, jnp.where(lane >= hi96, fold_right, zero(fold_rows))
        ),
    )

    fold_pairs = pack_pair(fold[0:4], fold[4:8])
    grad_gated = dot(mix_t, side_by_side([fold_wide[r] for r in range(10)]))
    sig_a = sigmoid(lin_a)
    slope_a_s[...] = sig_a * (1.0 + lin_a * (1.0 - sig_a))

    own_rows = slice(2, 10)
    lane = lane_of(coarse.shape)
    scb[own_rows, 0:32, :] = jnp.where(lane < 64, zero(coarse), roll(coarse, 32))
    scb[own_rows, 32:64, :] = coarse
    scb[own_rows, 64:96, :] = jnp.where(lane < 64, roll(coarse, -32), zero(coarse))

    fine_windows_cols(sfa, rx)
    for r in range(16):
        sft[r] = sfa[r : r + 3].reshape(288, 128).T

    halo_c.wait_recv()
    cols, rim = halo_parts(rc)

    def two(*parts):
        return jnp.concatenate(parts, axis=0)

    left, right = two(cols[0], roll(cols[0], 64)), two(roll(cols[1], 64), cols[1])
    left = jnp.where(lane < lo64, left, zero(left))
    right = jnp.where(lane >= hi64, right, zero(right))
    scb[own_rows, 0:32, :] = jnp.where(lane < 64, left, scb[own_rows, 0:32, :])
    scb[own_rows, 32:64, :] = jnp.where(
        lane < 32, roll(left, -32), jnp.where(lane < 96, coarse, roll(right, 32))
    )
    scb[own_rows, 64:96, :] = jnp.where(lane < 64, scb[own_rows, 64:96, :], right)
    lane = lane_of((2, 32, 128))
    for k, at in ((0, 0), (3, 10)):
        rows = two(roll(rim[k], 32), roll(rim[k], -32))
        left, right = two(rim[k + 1], roll(rim[k + 1], 64)), two(roll(rim[k + 2], 64), rim[k + 2])
        left = jnp.where(lane < lo64, left, zero(left))
        right = jnp.where(lane >= hi64, right, zero(right))
        scb[at : at + 2, 0:32, :] = jnp.where(lane < 64, left, roll(rows, 32))
        scb[at : at + 2, 32:64, :] = jnp.where(
            lane < 32, roll(left, -32), jnp.where(lane < 96, rows, roll(right, 32))
        )
        scb[at : at + 2, 64:96, :] = jnp.where(lane < 64, roll(rows, -32), right)

    conv_rows(scb, 10, wb_f, 64, lin_b_s)
    lin_b = lin_b_s[...]
    sig_b = sigmoid(lin_b)
    slope_b = sig_b * (1.0 + lin_b * (1.0 - sig_b))
    gated = (lin_b * sig_b)[1:9].astype(BF)
    grad_b = jnp.concatenate(
        [(grad_gated[:, 128 * r : 128 * (r + 1)] * slope_b[r]).astype(BF)[None] for r in range(10)],
        axis=0,
    )
    top, low = grad_b[0:6], grad_b[4:10]
    lane = lane_of(top.shape)
    sgb[:, 0:64, :] = jnp.where(lane < 64, top, roll(low, 64))
    sgb[:, 64:128, :] = pack_pair(top, low)
    sgb[:, 128:192, :] = jnp.where(lane < 64, roll(top, 64), low)

    shifts = layer_shifts(sgb[1:5, 64:128, :])
    up = side_by_side([jnp.concatenate([s[r] for s in shifts], axis=0) for r in range(4)])
    seen = pack_pair(scb[1:7], scb[5:11])
    seen = side_by_side([seen[r : r + 3].reshape(288, 128) for r in range(4)])
    gated = pack_pair(gated[0:4], gated[4:8])
    sum_b = dot_nt(seen, up)
    sum_m = dot_nt(
        side_by_side([fold_pairs[r] for r in range(4)]), side_by_side([gated[r] for r in range(4)])
    )
    for i in range(18):
        pb[i] = sum_b[16 * i : 16 * i + 16, 0:128].astype(BF)
    rest = side_by_side([sum_b[144 * g : 144 * g + 144, 128:192] for g in range(2)])
    for i in range(9):
        pb[18 + i] = rest[16 * i : 16 * i + 16].astype(BF)
    pb[27] = side_by_side([sum_m[0:16], sum_m[16:32]]).astype(BF)

    def spread(buf, dst, k):
        for i, step in enumerate(steps):
            q = plane_p[step[0]] * n_eta + eta_of[step[1]]
            send(buf.at[q], dst.at[i], s_send.at[k], s_recv.at[k], plane_device(step))
        copy = whole(dst, s_send.at[k], s_recv.at[k])
        departures.append(copy)
        return copy

    spread_b = spread(pb, rb, 0)

    conv_rows(sgb, 4, wb_b, 32, gc_s)
    grad_coarse = widen_pairs(gc_s[...].astype(BF).astype(F32))
    grad_hidden = jnp.concatenate(
        [(ct[:, i] + 0.25 * grad_coarse)[:, None] for i in range(2)], axis=1
    ).reshape(16, 32, 128)
    grad_a = (grad_hidden * slope_a_s[...]).astype(BF)
    g_s[...] = grad_a
    shifts = layer_shifts(grad_a)
    up = side_by_side([jnp.concatenate([s[r] for s in shifts], axis=0) for r in range(16)])
    sum_a = dot(up, sft[...].reshape(2048, 288))
    for i in range(12):
        for l in range(2):
            pa[2 * i + l] = sum_a[8 * i : 8 * i + 8, 128 * l : 128 * l + 128].astype(BF)
    rest = side_by_side([sum_a[32 * g : 32 * g + 32, 256:288] for g in range(3)])
    rest = jnp.concatenate([rest, jnp.zeros((32, 32), F32)], axis=1)
    for i in range(4):
        pa[24 + i] = rest[8 * i : 8 * i + 8].astype(BF)
    spread_a = spread(pa, ra, 1)
    colg_s[0] = pack_column(grad_a, 4, 96)
    colg_s[1] = pack_column(grad_a, 4, 0)
    def cross(copy, buf, arrived, mine, slots, k):
        copy.wait_recv()
        total = buf[me1].astype(F32)
        for i in range(g1 - 1):
            total = total + arrived[i].astype(F32)
        total = total.astype(BF)
        mine[...] = total
        slots[me2] = total
        for i in range(1, g2):
            send(mine, slots.at[me2], s_send.at[k], s_recv.at[k], line_device(i))
        copy = whole(slots.at[pl.ds(0, g2 - 1)], s_send.at[k], s_recv.at[k])
        departures.append(copy)
        return copy

    def gather(copy, slots, mine, result, k):
        copy.wait_recv()
        total = slots[0].astype(F32)
        for i in range(1, g2):
            total = total + slots[i].astype(F32)
        total = total.astype(BF)
        mine[...] = total
        result[me1] = total
        for step in steps:
            send(mine, result.at[me1], s_send.at[k], s_recv.at[k], plane_device(step))
        copy = whole(result.at[pl.ds(0, g1 - 1)], s_send.at[k], s_recv.at[k])
        departures.append(copy)
        return copy

    cross_b = cross(spread_b, pb, rb, xb2, rb2, 2)
    cross_a = cross(spread_a, pa, ra, xa2, ra2, 3)
    halo_g = halo_start(
        3, (colg_s.at[0], colg_s.at[1]), (g_s.at[15], g_s.at[0]), rg
    )

    projected = dot(mix, side_by_side([gated[r] for r in range(4)])).astype(BF).astype(F32)
    projected = jnp.concatenate(
        [projected[:, 128 * r : 128 * (r + 1)][None] for r in range(4)], axis=0
    )
    projected = widen_pairs(projected)
    output = jnp.concatenate(
        [(hidden[:, i] + projected)[:, None] for i in range(2)], axis=1
    ).reshape(16, 32, 128)
    out_ref[...] = jnp.transpose(output.astype(BF), (1, 0, 2))

    gather_b = gather(cross_b, rb2, xb3, resb, 4)
    gather_a = gather(cross_a, ra2, xa3, resa, 5)

    fine_windows_own(sga, grad_a)
    halo_g.wait_recv()
    fine_windows_cols(sga, rg)
    fine_windows_rows(sga, rg)
    conv_rows(sga, 16, wa_b, 32, gi_s)
    gi_ref[...] = jnp.transpose(gi_s[...].astype(BF), (1, 0, 2))

    gather_b.wait_recv()
    for ab in range(9):
        for h in range(2):
            rows = slice(16 * h, 16 * h + 16)
            u = 2 * ab + h
            pair = resb[u].astype(F32) * scale
            gkb_ref[3 * ab, rows, :] = pair[:, 0:64]
            gkb_ref[3 * ab + 1, rows, :] = pair[:, 64:128]
            g = u // 9
            rest = resb[18 + u % 9].astype(F32) * scale
            gkb_ref[3 * ab + 2, rows, :] = rest[:, 64 * g : 64 * g + 64]
    last = resb[27].astype(F32) * scale
    gm_ref[0:16, :] = last[:, 0:64]
    gm_ref[16:32, :] = last[:, 64:128]

    gather_a.wait_recv()
    for c in range(3):
        for h in range(4):
            rows = slice(8 * h, 8 * h + 8)
            for l in range(2):
                block = resa[2 * (4 * c + h) + l].astype(F32) * scale
                for q in range(4):
                    gka_ref[(4 * l + q) * 3 + c, rows, :] = block[:, 32 * q : 32 * q + 32]
            rest = resa[24 + h].astype(F32) * scale
            gka_ref[24 + c, rows, :] = rest[:, 32 * c : 32 * c + 32]

    for copy in departures:
        copy.wait_send()


def writer(*refs):
    sems = refs[10]
    copies = [
        pltpu.make_async_copy(src, dst, sems.at[k])
        for k, (src, dst) in enumerate(zip(refs[:5], refs[5:10]))
    ]
    for copy in copies:
        copy.start()
    for copy in copies:
        copy.wait()


def shards(n_phi, n_eta, features, cotangent, kernel_a, kernel_b, mixing):
    g1, g2 = 4 * n_eta, n_phi // 4
    assert g1 == PLANE
    cells = features.shape[1] * features.shape[2] * n_phi * n_eta
    kernel_b = jnp.swapaxes(kernel_b, 1, 2)
    ins = (features, cotangent, kernel_a, kernel_b, mixing)
    types = (BF, BF, F32, F32, F32)

    def vm(*shape, dtype=BF):
        return pltpu.VMEM(shape, dtype)

    def sums(n):
        return [
            vm(g1, n, 128), vm(g1 - 1, n, 128), vm(n, 128),
            vm(g2, n, 128), vm(n, 128), vm(g1, n, 128),
        ]

    def halo(n):
        return [vm(2 * n + 6, 32, 128)]

    dma = pltpu.SemaphoreType.DMA
    scratch = [
        *[vm(*a.shape) for a in ins], dma((5,)),
        vm(16, 32, 128), vm(2, 4, 32, 128), *halo(4),
        vm(8, 32, 128), vm(2, 2, 32, 128), *halo(2),
        vm(4, 32, 128), vm(2, 32, 128), *halo(4),
        vm(16, 32, 128), vm(2, 4, 32, 128), *halo(4),
        vm(18, 96, 128), vm(16, 128, 288), vm(12, 96, 128), vm(6, 192, 128), vm(18, 96, 128),
        vm(16, 32, 128, dtype=F32), vm(16, 32, 128, dtype=F32), vm(10, 64, 128, dtype=F32),
        vm(4, 32, 128, dtype=F32), vm(16, 32, 128, dtype=F32),
        *sums(8), *sums(16),
        *[dma((k,)) for k in (4, 4, 6, 6)],
    ]
    vmem = pl.BlockSpec(memory_space=pltpu.VMEM)
    anywhere = pl.BlockSpec(memory_space=pl.ANY)
    shapes = [a.shape for a in ins]
    outs = pl.pallas_call(
        functools.partial(kernel, n_phi, n_eta, 1.0 / math.sqrt(cells)),
        out_shape=tuple(pltpu.VMEM(s, t) for s, t in zip(shapes, types)),
        in_specs=[anywhere] * 5,
        out_specs=(vmem,) * 5,
        scratch_shapes=scratch,
        compiler_params=pltpu.CompilerParams(collective_id=0, has_side_effects=True),
        name="block_step",
    )(*ins)
    outs = pl.pallas_call(
        writer,
        out_shape=tuple(jax.ShapeDtypeStruct(s, t) for s, t in zip(shapes, types)),
        in_specs=[vmem] * 5,
        out_specs=(anywhere,) * 5,
        scratch_shapes=[dma((5,))],
        name="write_out",
    )(*[pltpu.with_memory_space_constraint(o, pltpu.VMEM) for o in outs])
    return (*outs[:3], jnp.swapaxes(outs[3], 1, 2), outs[4])


def solution(mesh):
    specs = (P(None, "phi", "eta"), P(None, "phi", "eta"), P(), P(), P())
    body = functools.partial(shards, mesh.shape["phi"], mesh.shape["eta"])
    return jax.shard_map(body, mesh=mesh, in_specs=specs, out_specs=specs, check_vma=False)
```
